32 devices in a mesh: dp: 2 (over x), row: 4 (over y, core), col: 4 (over z).
Axes of the slice: x: 2, y: 2, z: 4, core: 2. Of those that a mesh axis runs over, the one named last changes fastest.
Arguments:
- inputs: bfloat16 [12288, 4, 384], P(('dp', 'row'), 'col'), may hold values from -6 to 6
- segment_ids: int32 [24576], P(('dp', 'row')), may hold values from 0 to 95, never falling along the last dimension, each value on 1 to 800 neighbouring positions
- keep_mask: int32 [24576], P(('dp', 'row')), may hold values from 0 to 1, as said below
- query_weight: bfloat16 [768, 192], P('col', 'row'), may hold values from -0.4375 to 0.4375
- query_bias: float32 [768], P('col'), may hold values from -3 to 3
- key_weight: bfloat16 [768, 192], P('col', 'row'), may hold values from -0.4375 to 0.4375
- value_weight: bfloat16 [768, 192], P('col', 'row'), may hold values from -0.4375 to 0.4375
- value_bias: float32 [768], P('col'), may hold values from -3 to 3
- output_weight: bfloat16 [768, 768], P('col', 'row'), may hold values from -0.875 to 0.875
- output_bias: float32 [768], P('col'), may hold values from -3 to 3
- first_gain: float32 [768], P('col'), may hold values from 0.5 to 1.5
- first_shift: float32 [768], P('col'), may hold values from -3 to 3
- expand_weight: bfloat16 [768, 768], P('col', 'row'), may hold values from -0.4375 to 0.4375
- expand_bias: float32 [3072], P('col'), may hold values from -3 to 3
- reduce_weight: bfloat16 [3072, 192], P('col', 'row'), may hold values from -0.21875 to 0.21875
- reduce_bias: float32 [768], P('col'), may hold values from -3 to 3
- second_gain: float32 [768], P('col'), may hold values from 0.5 to 1.5
- second_shift: float32 [768], P('col'), may hold values from -3 to 3
- cotangent: bfloat16 [12288, 4, 384], P(('dp', 'row'), 'col'), may hold values from -6 to 6
Outputs:
- output: bfloat16 [12288, 4, 384], P(('dp', 'row'), 'col')
- input_grad: float32 [12288, 4, 384], P(('dp', 'row'), 'col')
- query_weight_grad: float32 [768, 192], P('col', 'row')
- query_bias_grad: float32 [768], P('col')
- key_weight_grad: float32 [768, 192], P('col', 'row')
- value_weight_grad: float32 [768, 192], P('col', 'row')
- value_bias_grad: float32 [768], P('col')
- output_weight_grad: float32 [768, 768], P('col', 'row')
- output_bias_grad: float32 [768], P('col')
- first_gain_grad: float32 [768], P('col')
- first_shift_grad: float32 [768], P('col')
- expand_weight_grad: float32 [768, 768], P('col', 'row')
- expand_bias_grad: float32 [3072], P('col')
- reduce_weight_grad: float32 [3072, 192], P('col', 'row')
- reduce_bias_grad: float32 [768], P('col')
- second_gain_grad: float32 [768], P('col')
- second_shift_grad: float32 [768], P('col')
The draws below stay inside these ranges and needn't reach their ends.
Inputs may be any that keep to these rules, and one draw needn't show every extreme that they name: `segment_ids`: along the tokens the number never falls; each document holds 1 to 800 tokens and one holds exactly 800; a document may run on into the next sequence. `keep_mask`: in each sequence of 1024 tokens the real tokens come first, 512 of them or more.
All inputs are finite; a program needn't handle non-finite values.
Results may differ from the reference program's by a relative error of at most 0.02.
Values may be sent and summed in bfloat16 or wider, within the bound.
A program may use at most 128 MiB of HBM per device.

```python
import math
import jax
import jax.numpy as jnp
import numpy as np
from jax import lax

D = 768
HEADS = 12
HEAD_DIM = 64
FF = 3072
GROUPS = 4
LEN = 1024
DOC_MOST = 800
TOKENS = 24576
DOCS = 96


def draw_keep_mask(key, part):
    filled = jax.random.randint(key, (TOKENS // LEN,), LEN // 2, LEN + 1)
    places = jnp.arange(TOKENS, dtype=jnp.int32)
    return (places % LEN < filled[places // LEN]).astype(jnp.int32)


def levels(rng, extent, cuts, smallest, top_value):
    loudness, own = 1.0, jax.random.fold_in(rng, 6)
    for position, shards_of in cuts:
        heights = jnp.exp(jax.random.uniform(jax.random.fold_in(own, position), (shards_of,), jnp.float32, smallest / len(cuts), top_value / len(cuts)))
        loudness = loudness * jnp.repeat(heights, extent[position] // shards_of).reshape([-1 if axis == position else 1 for axis in range(len(extent))])
    return loudness


def split_up(count, total, limit, slope):
    weights = [(1 << 20) // math.isqrt(standing ** slope) + 1 for standing in range(2, count + 1)]
    spare, given = total - limit - (count - 1), [1] * (count - 1)
    while spare > 0:
        free = [i for i in range(count - 1) if given[i] < limit]
        whole, budget = sum([weights[i] for i in free]), spare
        for i in free:
            more = min(limit - given[i], max(1, budget * weights[i] // whole), spare)
            given[i] = given[i] + more
            spare = spare - more
    return np.array([limit] + given)


def uneven_parts(own_key, number_of, total, bound, lean):
    if number_of == 2:
        one = jax.random.randint(own_key, (), max(1, total - bound), min(bound, total - 1) + 1)
        return jnp.stack([one, total - one])
    tallies = jnp.asarray(split_up(number_of, total, bound, lean), jnp.int32)
    twos = (number_of - 1) // 2
    giver, taker = tallies[1:1 + 2 * twos:2], tallies[2:2 + 2 * twos:2]
    room = jnp.minimum(giver - 1, bound - taker)
    moved = jax.random.randint(jax.random.fold_in(own_key, 1), (twos,), 0, 1 << 20) % (room + 1)
    tallies = tallies.at[1:1 + 2 * twos:2].set(giver - moved).at[2:2 + 2 * twos:2].set(taker + moved)
    return tallies[jax.random.permutation(jax.random.fold_in(own_key, 2), number_of)]


def gaussian(key, extent, deviation, limit, shards=(), kind=jnp.bfloat16):
    drawn = deviation * jax.random.normal(key, extent, jnp.float32)
    if shards:
        drawn = drawn * levels(key, extent, shards, -0.22, 0.18)
    return jnp.clip(drawn, -limit, limit).astype(kind)


def setup_inputs(seed: int = 0) -> dict:
    seeds = jax.random.split(jax.random.key(seed), 20)
    inputs = gaussian(seeds[0], (TOKENS // 2, GROUPS, 2 * D // GROUPS), 1.0, 6.0, ((0, 8), (1, 4)))
    segment_ids = jnp.searchsorted(jnp.cumsum(uneven_parts(seeds[1], DOCS, TOKENS, DOC_MOST, 1)), jnp.arange(TOKENS), side="right").astype(jnp.int32)
    keep_mask = draw_keep_mask(jax.random.fold_in(seeds[19], 71), 0)
    query_weight = gaussian(seeds[3], (D, D // GROUPS), (D // GROUPS) ** -0.5, 0.4375, ((0, 4), (1, 4)))
    query_bias = gaussian(seeds[4], (D,), 0.5, 3.0, ((0, 4),), jnp.float32)
    key_weight = gaussian(seeds[5], (D, D // GROUPS), (D // GROUPS) ** -0.5, 0.4375, ((0, 4), (1, 4)))
    value_weight = gaussian(seeds[6], (D, D // GROUPS), (D // GROUPS) ** -0.5, 0.4375, ((0, 4), (1, 4)))
    value_bias = gaussian(seeds[7], (D,), 0.5, 3.0, ((0, 4),), jnp.float32)
    output_weight = gaussian(seeds[8], (D, D), (D // 16) ** -0.5, 0.875, ((0, 4), (1, 4)))
    output_bias = gaussian(seeds[9], (D,), 0.5, 3.0, ((0, 4),), jnp.float32)
    first_gain = jnp.clip(1.0 + 0.1 * jax.random.normal(seeds[10], (D,), jnp.float32), 0.5, 1.5)
    first_shift = gaussian(seeds[11], (D,), 0.5, 3.0, ((0, 4),), jnp.float32)
    expand_weight = gaussian(seeds[12], (D, FF // GROUPS), (D // GROUPS) ** -0.5, 0.4375, ((0, 4), (1, 4)))
    expand_bias = gaussian(seeds[13], (FF,), 0.5, 3.0, ((0, 4),), jnp.float32)
    reduce_weight = gaussian(seeds[14], (FF, D // GROUPS), (FF // GROUPS) ** -0.5, 0.21875, ((0, 4), (1, 4)))
    reduce_bias = gaussian(seeds[15], (D,), 0.5, 3.0, ((0, 4),), jnp.float32)
    second_gain = jnp.clip(1.0 + 0.1 * jax.random.normal(seeds[16], (D,), jnp.float32), 0.5, 1.5)
    second_shift = gaussian(seeds[17], (D,), 0.5, 3.0, ((0, 4),), jnp.float32)
    cotangent = gaussian(seeds[18], (TOKENS // 2, GROUPS, 2 * D // GROUPS), 1.0, 6.0, ((0, 8), (1, 4)))
    return dict(inputs=inputs, segment_ids=segment_ids, keep_mask=keep_mask, query_weight=query_weight, query_bias=query_bias, key_weight=key_weight, value_weight=value_weight, value_bias=value_bias, output_weight=output_weight, output_bias=output_bias, first_gain=first_gain, first_shift=first_shift, expand_weight=expand_weight, expand_bias=expand_bias, reduce_weight=reduce_weight, reduce_bias=reduce_bias, second_gain=second_gain, second_shift=second_shift, cotangent=cotangent)


EPSILON = 1e-05
NEGATIVE = -1e+30
EXACTNESS = lax.Precision.HIGHEST

@jax.custom_vjp
def low(v):
    return lax.optimization_barrier(v.astype(jnp.bfloat16)).astype(jnp.float32)

@jax.custom_vjp
def low_back(v):
    return v

def low_keep(v):
    return (low(v), None)

def low_pass(kept, grad):
    return (grad,)

def back_keep(v):
    return (v, None)

def back_low(kept, grad):
    return (low(grad),)
low.defvjp(low_keep, low_pass)
low_back.defvjp(back_keep, back_low)

def unpair(paired):
    first, blocks, width = paired.shape
    split = paired.reshape(first, blocks, 2, width // 2)
    return jnp.transpose(split, (0, 2, 1, 3)).reshape(first * 2, blocks * (width // 2))

def pair_up(matrix, blocks):
    count, width = matrix.shape
    split = matrix.reshape(count // 2, 2, blocks, width // blocks)
    return jnp.transpose(split, (0, 2, 1, 3)).reshape(count // 2, blocks, 2 * (width // blocks))

def grouped(features, weight):
    row_count = features.shape[0]
    group_width = features.shape[1] // GROUPS
    pieces = features.reshape(row_count, GROUPS, group_width)
    blocks = weight.reshape(GROUPS, group_width, weight.shape[1])
    joined = jnp.einsum('tgi,gio->tgo', pieces, blocks, precision=EXACTNESS)
    return joined.reshape(row_count, GROUPS * weight.shape[1])

def layer_norm(summed, norm_gain, norm_shift):
    center = lax.optimization_barrier(jnp.mean(summed, axis=-1, keepdims=True))
    spread = lax.optimization_barrier(jnp.mean((summed - center) ** 2, axis=-1, keepdims=True))
    return (summed - center) * lax.rsqrt(spread + EPSILON) * norm_gain + norm_shift

def attend(queries, key_rows, value_rows, segment, keep_mask):
    block_rows = min(512, LEN)
    score_scale = HEAD_DIM ** (-0.5)
    positions = jnp.arange(LEN, dtype=jnp.int32)

    def one_block(block_index):
        offset = block_index * block_rows
        block_queries = lax.dynamic_slice_in_dim(queries, offset, block_rows, 1)
        block_segment = lax.dynamic_slice_in_dim(segment, offset, block_rows, 1)
        block_positions = offset + jnp.arange(block_rows, dtype=jnp.int32)
        same_segment = block_segment[:, :, None] == segment[:, None, :]
        usable = (keep_mask[:, None, :] == 1) | (block_positions[:, None] == positions[None, :])[None]
        allowed = same_segment & usable
        scores = low_back(jnp.einsum('nqhd,nkhd->nhqk', block_queries, key_rows, precision=EXACTNESS) * score_scale)
        masked = jnp.where(allowed[:, None], scores, NEGATIVE)
        highest = lax.optimization_barrier(jnp.max(masked, axis=-1, keepdims=True))
        exponent = jnp.exp(masked - highest)
        weights = exponent / lax.optimization_barrier(jnp.sum(exponent, axis=-1, keepdims=True))
        return jnp.einsum('nhqk,nkhd->nqhd', low(weights), value_rows, precision=EXACTNESS)
    pieces = lax.map(jax.checkpoint(one_block), jnp.arange(LEN // block_rows, dtype=jnp.int32))
    moved = jnp.moveaxis(pieces, 0, 1)
    return moved.reshape(queries.shape)

def forward(inputs, query_weight, query_bias, key_weight, value_weight, value_bias, output_weight, output_bias, first_gain, first_shift, expand_weight, expand_bias, reduce_weight, reduce_bias, second_gain, second_shift, segment, keep_mask):
    row_count = inputs.shape[0]
    sequences = row_count // LEN
    layout = (sequences, LEN, HEADS, HEAD_DIM)
    queries = low(low_back(grouped(inputs, query_weight) + query_bias))
    key_rows = low(low_back(grouped(inputs, key_weight)))
    value_rows = low(low_back(grouped(inputs, value_weight) + value_bias))
    context = attend(queries.reshape(layout), key_rows.reshape(layout), value_rows.reshape(layout), segment.reshape(sequences, LEN), keep_mask.reshape(sequences, LEN))
    context = low(low_back(context.reshape(row_count, D)))
    attended = low_back(jnp.dot(context, output_weight, precision=EXACTNESS))
    middle = layer_norm(inputs + attended + output_bias, first_gain, first_shift)
    expanded = low_back(grouped(low(middle), expand_weight) + expand_bias)
    activated = low(jax.nn.gelu(expanded, approximate=False))
    reduced = low_back(grouped(activated, reduce_weight))
    return layer_norm(middle + reduced + reduce_bias, second_gain, second_shift)

def reference(inputs, segment_ids, keep_mask, query_weight, query_bias, key_weight, value_weight, value_bias, output_weight, output_bias, first_gain, first_shift, expand_weight, expand_bias, reduce_weight, reduce_bias, second_gain, second_shift, cotangent):
    params = tuple((parameter.astype(jnp.float32) for parameter in (query_weight, query_bias, key_weight, value_weight, value_bias, output_weight, output_bias, first_gain, first_shift, expand_weight, expand_bias, reduce_weight, reduce_bias, second_gain, second_shift)))
    group_rows = 4 * LEN
    steps_count = TOKENS // group_rows
    input_rows = unpair(inputs.astype(jnp.float32))
    cotangent_rows = unpair(cotangent.astype(jnp.float32))
    stacked = (input_rows.reshape(steps_count, group_rows, D), segment_ids.reshape(steps_count, group_rows), keep_mask.reshape(steps_count, group_rows), cotangent_rows.reshape(steps_count, group_rows, D))
    starting = tuple((jnp.zeros(parameter.shape, jnp.float32) for parameter in params))

    def scan_step(totals, scan_item):
        block_inputs, block_segment, block_keep, block_cotangent = scan_item

        def apply_layer(layer_in, *weights):
            return forward(layer_in, *weights, block_segment, block_keep)
        result, pullback = jax.vjp(apply_layer, block_inputs, *params)
        gradients = pullback(block_cotangent)
        updated = tuple((running + fresh for running, fresh in zip(totals, gradients[1:])))
        return (updated, (result.astype(jnp.bfloat16), gradients[0]))
    totals, (outputs, input_grads) = lax.scan(scan_step, starting, stacked)
    layer_out = pair_up(outputs.reshape(TOKENS, D), GROUPS)
    input_grad = pair_up(input_grads.reshape(TOKENS, D), GROUPS)
    return (layer_out, input_grad, totals[0], totals[1], totals[2], totals[3], totals[4], totals[5], totals[6], totals[7], totals[8], totals[9], totals[10], totals[11], totals[12], totals[13], totals[14])
```

```python
import functools

import jax
import jax.numpy as jnp
from jax import lax
from jax.experimental import pallas as pl
from jax.experimental.pallas import tpu as pltpu
from jax.sharding import PartitionSpec as P

MESH = pl.DeviceIdType.MESH
BF16 = jnp.bfloat16
F32 = jnp.float32

D = 768
HEAD_DIM = 64
LEN = 1024
BLOCK = 256
PAIRS = BLOCK // 2
EPSILON = 1e-05
NEGATIVE = -1e30
ROOT_HALF = 0.7071067811865476
DENSITY_SCALE = 0.3989422804014327
VMEM_BYTES = 62 * 1024 * 1024


def dot(left, right):
    return jnp.dot(left, right, preferred_element_type=F32)


def dot_nt(left, right):
    return lax.dot_general(left, right, (((1,), (1,)), ((), ())), preferred_element_type=F32)


def columns_of(pairs):
    width = pairs.shape[1] // 2
    turned = pairs.T
    return jnp.concatenate([turned[:width], turned[width:]], axis=1)


def pairs_of(columns):
    half = columns.shape[1] // 2
    return jnp.concatenate([columns[:, :half], columns[:, half:]], axis=0).T


def vmem_spec():
    return pl.BlockSpec(memory_space=pltpu.VMEM)


def key_range(segment_ref, keep_ref, base, query_block, blocks):
    first = segment_ref[base + query_block * BLOCK]
    last = segment_ref[base + query_block * BLOCK + BLOCK - 1]
    low = jnp.int32(0)
    high = jnp.int32(-1)
    real = jnp.int32(-1)
    for block in range(blocks):
        low += (segment_ref[base + block * BLOCK + BLOCK - 1] < first).astype(jnp.int32)
        high += (segment_ref[base + block * BLOCK] <= last).astype(jnp.int32)
        real += (keep_ref[base + block * BLOCK] == 1).astype(jnp.int32)
    return low, jnp.minimum(high, jnp.maximum(real, query_block))


def block_bias(key_codes, codes_ref, query_block, key_block):
    keys = key_codes[pl.ds(pl.multiple_of(key_block * BLOCK, BLOCK), BLOCK), :]
    keys = jnp.concatenate([keys, keys], axis=1)
    queries = codes_ref[query_block, 0:1, :]
    place = lax.broadcasted_iota(jnp.int32, (BLOCK, BLOCK), 0) - lax.broadcasted_iota(
        jnp.int32, (BLOCK, BLOCK), 1
    )
    same = place == (query_block - key_block) * BLOCK
    return jnp.where((keys == queries) | same, 0.0, NEGATIVE)


def spread_key_codes(codes_ref, key_codes, blocks):
    for block in range(blocks):
        column = codes_ref[block].T[:, 1:2]
        key_codes[pl.ds(block * BLOCK, BLOCK), :] = jnp.broadcast_to(column, (BLOCK, 128))


def forward_kernel(
    segment_ref, keep_ref, inputs_ref, weight_ref, vectors_ref, codes_ref,
    turned_ref, joined_ref, context_ref, logsum_ref,
    key_codes, key_rows, value_rows, scaled, scores, totals, vector_columns,
):
    blocks = LEN // BLOCK
    base = pl.program_id(0) * LEN
    width = inputs_ref.shape[1] // 2
    heads = width // HEAD_DIM
    vector_columns[...] = vectors_ref[...].T
    spread_key_codes(codes_ref, key_codes, blocks)
    for block in range(blocks):
        turned = columns_of(inputs_ref[block * PAIRS : (block + 1) * PAIRS, :])
        turned_ref[block] = turned
        query = (dot(weight_ref[0], turned) + vector_columns[:, 0:1]).astype(BF16)
        key = dot(weight_ref[1], turned).astype(BF16)
        value = (dot(weight_ref[2], turned) + vector_columns[:, 1:2]).astype(BF16)
        joined_ref[block, 0] = query
        joined_ref[block, 1] = key
        joined_ref[block, 2] = value
        scaled[block] = query * jnp.array(HEAD_DIM ** (-0.5), BF16)
        for head in range(heads):
            rows = slice(head * HEAD_DIM, (head + 1) * HEAD_DIM)
            key_rows[head, block] = key[rows].T
            value_rows[head, block, :HEAD_DIM] = value[rows]
            value_rows[head, block, HEAD_DIM:] = jnp.ones((16, BLOCK), BF16)

    def query_step(query_block, carry):
        low, high = key_range(segment_ref, keep_ref, base, query_block, blocks)

        def score_step(key_block, highest):
            bias = block_bias(key_codes, codes_ref, query_block, key_block)
            fresh = []
            for head in range(heads):
                rows = slice(head * HEAD_DIM, (head + 1) * HEAD_DIM)
                score = dot(key_rows[head, key_block], scaled[query_block, rows, :]) + bias
                scores[head, key_block] = score
                fresh.append(
                    jnp.maximum(
                        highest[head], jnp.max(score.reshape(BLOCK // 8, 8, BLOCK), axis=0)
                    )
                )
            return tuple(fresh)

        start = jnp.full((8, BLOCK), 2 * NEGATIVE, F32)
        highest = lax.fori_loop(low, high + 1, score_step, (start,) * heads)
        highest = [jnp.max(part, axis=0, keepdims=True) for part in highest]
        totals[...] = jnp.zeros_like(totals)

        def value_step(key_block, carry):
            for head in range(heads):
                weights = jnp.exp(scores[head, key_block] - highest[head]).astype(BF16)
                totals[head] += dot(value_rows[head, key_block], weights)
            return carry

        lax.fori_loop(low, high + 1, value_step, 0)
        for head in range(heads):
            rows = slice(head * HEAD_DIM, (head + 1) * HEAD_DIM)
            total = totals[head, HEAD_DIM : HEAD_DIM + 1, :]
            context_ref[query_block, rows, :] = (totals[head, :HEAD_DIM, :] / total).astype(BF16)
            logsum_ref[query_block, head : head + 1, :] = highest[head] + jnp.log(total)
        return carry

    lax.fori_loop(0, blocks, query_step, 0)


def attention_forward(pairs, segment_ids, keep_mask, weight, vectors, codes):
    pair_count, doubled = pairs.shape
    width = doubled // 2
    heads = width // HEAD_DIM
    sequences = pair_count * 2 // LEN
    blocks = LEN // BLOCK
    every = sequences * blocks

    def whole(*shape):
        return pl.BlockSpec(shape, lambda i, *refs: (0,) * len(shape))

    def part(*shape):
        return pl.BlockSpec(shape, lambda i, *refs: (i,) + (0,) * (len(shape) - 1))

    return pl.pallas_call(
        forward_kernel,
        out_shape=(
            jax.ShapeDtypeStruct((every, width, BLOCK), BF16),
            jax.ShapeDtypeStruct((every, 3, width, BLOCK), BF16),
            jax.ShapeDtypeStruct((every, width, BLOCK), BF16),
            jax.ShapeDtypeStruct((every, 8, BLOCK), F32),
        ),
        grid_spec=pltpu.PrefetchScalarGridSpec(
            num_scalar_prefetch=2,
            grid=(sequences,),
            in_specs=[
                part(LEN // 2, doubled),
                whole(3, width, width),
                whole(*vectors.shape),
                part(blocks, 8, BLOCK),
            ],
            out_specs=(
                part(blocks, width, BLOCK),
                part(blocks, 3, width, BLOCK),
                part(blocks, width, BLOCK),
                part(blocks, 8, BLOCK),
            ),
            scratch_shapes=[
                pltpu.VMEM((LEN, 128), F32),
                pltpu.VMEM((heads, blocks, BLOCK, HEAD_DIM), BF16),
                pltpu.VMEM((heads, blocks, HEAD_DIM + 16, BLOCK), BF16),
                pltpu.VMEM((blocks, width, BLOCK), BF16),
                pltpu.VMEM((heads, blocks, BLOCK, BLOCK), F32),
                pltpu.VMEM((heads, HEAD_DIM + 16, BLOCK), F32),
                pltpu.VMEM((width, vectors.shape[0]), F32),
            ],
        ),
        compiler_params=pltpu.CompilerParams(vmem_limit_bytes=VMEM_BYTES),
        name="attention_forward",
    )(segment_ids, keep_mask, pairs, weight, vectors, codes)


def backward_kernel(
    segment_ref, keep_ref, turned_ref, joined_ref, context_ref, logsum_ref, upstream_ref,
    first_back_ref, weight_ref, codes_ref,
    input_grad_ref, weight_grad_ref, bias_grad_ref,
    key_codes, key_rows, value_rows, scaled, deltas, query_sum, key_sum, value_sum, weight_in,
):
    blocks = LEN // BLOCK
    step = pl.program_id(0)
    base = step * LEN
    width = turned_ref.shape[1]
    heads = width // HEAD_DIM
    scale = HEAD_DIM ** (-0.5)

    @pl.when(step == 0)
    def start():
        weight_grad_ref[...] = jnp.zeros_like(weight_grad_ref)
        bias_grad_ref[...] = jnp.zeros_like(bias_grad_ref)
        for kind in range(3):
            weight_in[kind] = weight_ref[kind].T

    spread_key_codes(codes_ref, key_codes, blocks)
    query_sum[...] = jnp.zeros_like(query_sum)
    key_sum[...] = jnp.zeros_like(key_sum)
    value_sum[...] = jnp.zeros_like(value_sum)
    for block in range(blocks):
        query = joined_ref[block, 0]
        scaled[block] = query * jnp.array(scale, BF16)
        product = upstream_ref[block].astype(F32) * context_ref[block].astype(F32)
        for head in range(heads):
            rows = slice(head * HEAD_DIM, (head + 1) * HEAD_DIM)
            key_rows[head, block] = joined_ref[block, 1, rows, :].T
            value_rows[head, block] = joined_ref[block, 2, rows, :].T
            deltas[block, head : head + 1, :] = jnp.sum(product[rows], axis=0, keepdims=True)

    def query_step(query_block, carry):
        low, high = key_range(segment_ref, keep_ref, base, query_block, blocks)

        def key_step(key_block, carry):
            bias = block_bias(key_codes, codes_ref, query_block, key_block)
            for head in range(heads):
                rows = slice(head * HEAD_DIM, (head + 1) * HEAD_DIM)
                query = scaled[query_block, rows, :]
                upstream = upstream_ref[query_block, rows, :]
                logsum = logsum_ref[query_block, head : head + 1, :]
                delta = deltas[query_block, head : head + 1, :]
                weights = jnp.exp(dot(key_rows[head, key_block], query) + bias - logsum)
                weight_back = dot(value_rows[head, key_block], upstream)
                score_back = (weights * (weight_back - delta)).astype(BF16)
                value_sum[key_block, rows, :] += dot_nt(upstream, weights.astype(BF16))
                key_sum[key_block, rows, :] += dot_nt(query, score_back)
                query_sum[query_block, rows, :] += dot(
                    joined_ref[key_block, 1, rows, :], score_back
                )
            return carry

        return lax.fori_loop(low, high + 1, key_step, carry)

    lax.fori_loop(0, blocks, query_step, 0)
    for block in range(blocks):
        query_low = (query_sum[block] * scale).astype(BF16)
        key_low = key_sum[block].astype(BF16)
        value_low = value_sum[block].astype(BF16)
        turned = turned_ref[block]
        weight_grad_ref[0] += dot_nt(query_low, turned)
        weight_grad_ref[1] += dot_nt(key_low, turned)
        weight_grad_ref[2] += dot_nt(value_low, turned)
        query_wide = query_low.astype(F32)
        value_wide = value_low.astype(F32)
        bias_grad_ref[0] += query_wide[:, :128] + query_wide[:, 128:]
        bias_grad_ref[1] += value_wide[:, :128] + value_wide[:, 128:]
        input_grad = (
            first_back_ref[block]
            + dot(weight_in[0], query_low)
            + dot(weight_in[1], key_low)
            + dot(weight_in[2], value_low)
        )
        input_grad_ref[block * PAIRS : (block + 1) * PAIRS, :] = pairs_of(input_grad)


def attention_backward(
    segment_ids, keep_mask, turned, joined, context, logsums, upstream, first_back, weight, codes
):
    every, width, unused = turned.shape
    heads = width // HEAD_DIM
    blocks = LEN // BLOCK
    sequences = every // blocks

    def whole(*shape):
        return pl.BlockSpec(shape, lambda i, *refs: (0,) * len(shape))

    def part(*shape):
        return pl.BlockSpec(shape, lambda i, *refs: (i,) + (0,) * (len(shape) - 1))

    return pl.pallas_call(
        backward_kernel,
        out_shape=(
            jax.ShapeDtypeStruct((sequences * LEN // 2, 2 * width), F32),
            jax.ShapeDtypeStruct((3, width, width), F32),
            jax.ShapeDtypeStruct((2, width, 128), F32),
        ),
        grid_spec=pltpu.PrefetchScalarGridSpec(
            num_scalar_prefetch=2,
            grid=(sequences,),
            in_specs=[
                part(blocks, width, BLOCK),
                part(blocks, 3, width, BLOCK),
                part(blocks, width, BLOCK),
                part(blocks, 8, BLOCK),
                part(blocks, width, BLOCK),
                part(blocks, width, BLOCK),
                whole(3, width, width),
                part(blocks, 8, BLOCK),
            ],
            out_specs=(
                part(LEN // 2, 2 * width),
                whole(3, width, width),
                whole(2, width, 128),
            ),
            scratch_shapes=[
                pltpu.VMEM((LEN, 128), F32),
                pltpu.VMEM((heads, blocks, BLOCK, HEAD_DIM), BF16),
                pltpu.VMEM((heads, blocks, BLOCK, HEAD_DIM), BF16),
                pltpu.VMEM((blocks, width, BLOCK), BF16),
                pltpu.VMEM((blocks, 8, BLOCK), F32),
                pltpu.VMEM((blocks, width, BLOCK), F32),
                pltpu.VMEM((blocks, width, BLOCK), F32),
                pltpu.VMEM((blocks, width, BLOCK), F32),
                pltpu.VMEM((3, width, width), BF16),
            ],
        ),
        compiler_params=pltpu.CompilerParams(vmem_limit_bytes=VMEM_BYTES),
        name="attention_backward",
    )(segment_ids, keep_mask, turned, joined, context, logsums, upstream, first_back, weight, codes)


def as_rows(paired):
    return paired.reshape(paired.shape[0] * 2, paired.shape[2] // 2)


def as_pairs(matrix):
    return matrix.reshape(matrix.shape[0] // 2, 1, matrix.shape[1] * 2)


def forward_product(left, right):
    return jnp.dot(left, right, preferred_element_type=jnp.float32)


def product_transposed(left, right):
    return lax.dot_general(
        left, right, (((1,), (1,)), ((), ())), preferred_element_type=jnp.float32
    )


def product_over_rows(left, right):
    return lax.dot_general(
        left, right, (((0,), (0,)), ((), ())), preferred_element_type=jnp.float32
    )


def norm_forward(summed, norm_gain, norm_shift):
    totals = lax.psum((jnp.sum(summed, axis=1), jnp.sum(summed * summed, axis=1)), "col")
    center = totals[0] / D
    inverse = lax.rsqrt(totals[1] / D - center * center + EPSILON)
    normal = (summed - center[:, None]) * inverse[:, None]
    return (normal * norm_gain + norm_shift, normal, inverse)


def norm_backward(upstream, normal, inverse, norm_gain):
    scaled = upstream * norm_gain
    totals = lax.psum((jnp.sum(scaled, axis=1), jnp.sum(scaled * normal, axis=1)), "col")
    back = inverse[:, None] * (scaled - totals[0][:, None] / D - normal * totals[1][:, None] / D)
    return (back, jnp.sum(upstream * normal, axis=0), jnp.sum(upstream, axis=0))


def rows_of(blocked):
    every, width, unused = blocked.shape
    return blocked.reshape(every, width, 2, PAIRS).transpose(0, 3, 2, 1).reshape(every * BLOCK, width)


def columns_from(rows):
    every, width = rows.shape[0] // BLOCK, rows.shape[1]
    return rows.reshape(every, PAIRS, 2, width).transpose(0, 3, 2, 1).reshape(every, width, BLOCK)


def spread(vector, row_devices):
    return jnp.broadcast_to(vector[:, None], (vector.shape[0], row_devices))


def local(
    inputs,
    segment_ids,
    keep_mask,
    query_weight,
    query_bias,
    key_weight,
    value_weight,
    value_bias,
    output_weight,
    output_bias,
    first_gain,
    first_shift,
    expand_weight,
    expand_bias,
    reduce_weight,
    reduce_bias,
    second_gain,
    second_shift,
    cotangent,
):
    pairs = inputs[:, 0, :]
    inputs = as_rows(inputs)
    cotangent = as_rows(cotangent)
    query_full, key_full, value_full, output_full, expand_full, reduce_full = (
        lax.all_gather(query_weight, "row", axis=1, tiled=True),
        lax.all_gather(key_weight, "row", axis=1, tiled=True),
        lax.all_gather(value_weight, "row", axis=1, tiled=True),
        lax.all_gather(output_weight, "row", axis=1, tiled=True),
        lax.all_gather(expand_weight, "row", axis=1, tiled=True),
        lax.all_gather(reduce_weight, "row", axis=1, tiled=True),
    )
    every = segment_ids.shape[0] // BLOCK
    coded = jnp.stack([segment_ids, jnp.where(keep_mask == 1, segment_ids, -1)]).astype(F32)
    coded = coded.reshape(2, every, PAIRS, 2).transpose(1, 0, 3, 2).reshape(every, 2, BLOCK)
    codes = jnp.pad(coded, ((0, 0), (0, 6), (0, 0)))
    weight = jnp.stack([query_full.T, key_full.T, value_full.T])
    vectors = jnp.pad(jnp.stack([query_bias, value_bias]), ((0, 6), (0, 0)))
    turned, joined, context_t, logsums = attention_forward(pairs, segment_ids, keep_mask, weight, vectors, codes)
    context = rows_of(context_t)
    attended = lax.psum_scatter(
        forward_product(context, output_full).astype(jnp.bfloat16),
        "col",
        scatter_dimension=1,
        tiled=True,
    ).astype(jnp.float32)
    middle, first_normal, first_inverse = norm_forward(
        inputs.astype(jnp.float32) + attended + output_bias, first_gain, first_shift
    )
    middle_low = middle.astype(jnp.bfloat16)
    expanded = forward_product(middle_low, expand_full) + expand_bias
    activated = jax.nn.gelu(expanded, approximate=False).astype(jnp.bfloat16)
    reduced = forward_product(activated, reduce_full)
    result, second_normal, second_inverse = norm_forward(
        middle + reduced + reduce_bias, second_gain, second_shift
    )
    second_back, gain_second, shift_second = norm_backward(
        cotangent.astype(jnp.float32), second_normal, second_inverse, second_gain
    )
    bias_reduce = jnp.sum(second_back, axis=0)
    reduced_back = second_back.astype(jnp.bfloat16)
    activated_back = product_transposed(reduced_back, reduce_full)
    grad_reduce = product_over_rows(activated, reduced_back)
    gelu_slope = 0.5 * (1.0 + lax.erf(expanded * ROOT_HALF)) + expanded * DENSITY_SCALE * jnp.exp(
        -0.5 * expanded * expanded
    )
    expanded_back = (activated_back * gelu_slope).astype(jnp.bfloat16)
    bias_expand = jnp.sum(expanded_back.astype(jnp.float32), axis=0)
    grad_expand = product_over_rows(middle_low, expanded_back)
    middle_back = second_back + product_transposed(expanded_back, expand_full)
    first_back, gain_first, shift_first = norm_backward(
        middle_back, first_normal, first_inverse, first_gain
    )
    bias_output = jnp.sum(first_back, axis=0)
    attended_back = first_back.astype(jnp.bfloat16)
    upstream_whole = lax.all_gather(attended_back, "col", axis=1, tiled=True)
    context_grad = product_transposed(upstream_whole, output_full)
    grad_output = product_over_rows(context, upstream_whole)
    input_grad, weight_grad, bias_grad = attention_backward(
        segment_ids, keep_mask, turned, joined, context_t, logsums, columns_from(context_grad.astype(BF16)),
        columns_from(first_back), weight, codes)
    bias_query = jnp.sum(bias_grad[0], axis=1)
    bias_value = jnp.sum(bias_grad[1], axis=1)
    grad_query, grad_key, grad_value = weight_grad[0].T, weight_grad[1].T, weight_grad[2].T
    row_devices = lax.axis_size("row")
    scattered = (
        lax.psum_scatter(
            grad_query.astype(jnp.bfloat16), "row", scatter_dimension=1, tiled=True
        ).astype(jnp.float32),
        lax.psum_scatter(
            grad_key.astype(jnp.bfloat16), "row", scatter_dimension=1, tiled=True
        ).astype(jnp.float32),
        lax.psum_scatter(
            grad_value.astype(jnp.bfloat16), "row", scatter_dimension=1, tiled=True
        ).astype(jnp.float32),
        lax.psum_scatter(
            grad_output.astype(jnp.bfloat16), "row", scatter_dimension=1, tiled=True
        ).astype(jnp.float32),
        lax.psum_scatter(
            grad_expand.astype(jnp.bfloat16), "row", scatter_dimension=1, tiled=True
        ).astype(jnp.float32),
        lax.psum_scatter(
            grad_reduce.astype(jnp.bfloat16), "row", scatter_dimension=1, tiled=True
        ).astype(jnp.float32),
        lax.psum_scatter(
            spread(bias_query, row_devices).astype(jnp.bfloat16),
            "row",
            scatter_dimension=1,
            tiled=True,
        ).astype(jnp.float32),
        lax.psum_scatter(
            spread(bias_value, row_devices).astype(jnp.bfloat16),
            "row",
            scatter_dimension=1,
            tiled=True,
        ).astype(jnp.float32),
        lax.psum_scatter(
            spread(bias_output, row_devices).astype(jnp.bfloat16),
            "row",
            scatter_dimension=1,
            tiled=True,
        ).astype(jnp.float32),
        lax.psum_scatter(
            spread(gain_first, row_devices).astype(jnp.bfloat16),
            "row",
            scatter_dimension=1,
            tiled=True,
        ).astype(jnp.float32),
        lax.psum_scatter(
            spread(shift_first, row_devices).astype(jnp.bfloat16),
            "row",
            scatter_dimension=1,
            tiled=True,
        ).astype(jnp.float32),
        lax.psum_scatter(
            spread(bias_expand, row_devices).astype(jnp.bfloat16),
            "row",
            scatter_dimension=1,
            tiled=True,
        ).astype(jnp.float32),
        lax.psum_scatter(
            spread(bias_reduce, row_devices).astype(jnp.bfloat16),
            "row",
            scatter_dimension=1,
            tiled=True,
        ).astype(jnp.float32),
        lax.psum_scatter(
            spread(gain_second, row_devices).astype(jnp.bfloat16),
            "row",
            scatter_dimension=1,
            tiled=True,
        ).astype(jnp.float32),
        lax.psum_scatter(
            spread(shift_second, row_devices).astype(jnp.bfloat16),
            "row",
            scatter_dimension=1,
            tiled=True,
        ).astype(jnp.float32),
    )
    summed = (
        lax.psum(scattered[0].astype(jnp.bfloat16), "dp").astype(jnp.float32),
        lax.psum(scattered[1].astype(jnp.bfloat16), "dp").astype(jnp.float32),
        lax.psum(scattered[2].astype(jnp.bfloat16), "dp").astype(jnp.float32),
        lax.psum(scattered[3].astype(jnp.bfloat16), "dp").astype(jnp.float32),
        lax.psum(scattered[4].astype(jnp.bfloat16), "dp").astype(jnp.float32),
        lax.psum(scattered[5].astype(jnp.bfloat16), "dp").astype(jnp.float32),
        lax.psum(scattered[6][:, 0].astype(jnp.bfloat16), "dp").astype(jnp.float32),
        lax.psum(scattered[7][:, 0].astype(jnp.bfloat16), "dp").astype(jnp.float32),
        lax.psum(scattered[8][:, 0].astype(jnp.bfloat16), "dp").astype(jnp.float32),
        lax.psum(scattered[9][:, 0].astype(jnp.bfloat16), "dp").astype(jnp.float32),
        lax.psum(scattered[10][:, 0].astype(jnp.bfloat16), "dp").astype(jnp.float32),
        lax.psum(scattered[11][:, 0].astype(jnp.bfloat16), "dp").astype(jnp.float32),
        lax.psum(scattered[12][:, 0].astype(jnp.bfloat16), "dp").astype(jnp.float32),
        lax.psum(scattered[13][:, 0].astype(jnp.bfloat16), "dp").astype(jnp.float32),
        lax.psum(scattered[14][:, 0].astype(jnp.bfloat16), "dp").astype(jnp.float32),
    )
    return (
        as_pairs(result.astype(jnp.bfloat16)),
        input_grad[:, None, :],
        summed[0],
        summed[6],
        summed[1],
        summed[2],
        summed[7],
        summed[3],
        summed[8],
        summed[9],
        summed[10],
        summed[4],
        summed[11],
        summed[5],
        summed[12],
        summed[13],
        summed[14],
    )


def solution(mesh):
    placed = (
        P(("dp", "row"), "col", None),
        P(("dp", "row")),
        P(("dp", "row")),
        P("col", "row"),
        P("col"),
        P("col", "row"),
        P("col", "row"),
        P("col"),
        P("col", "row"),
        P("col"),
        P("col"),
        P("col"),
        P("col", "row"),
        P("col"),
        P("col", "row"),
        P("col"),
        P("col"),
        P("col"),
        P(("dp", "row"), "col", None),
    )
    return jax.shard_map(
        local,
        mesh=mesh,
        in_specs=placed,
        out_specs=(
            P(("dp", "row"), "col", None),
            P(("dp", "row"), "col", None),
            P("col", "row"),
            P("col"),
            P("col", "row"),
            P("col", "row"),
            P("col"),
            P("col", "row"),
            P("col"),
            P("col"),
            P("col"),
            P("col", "row"),
            P("col"),
            P("col", "row"),
            P("col"),
            P("col"),
            P("col"),
        ),
        check_vma=False,
    )
```

```python
import functools

import jax
import jax.numpy as jnp
from jax import lax
from jax.experimental import pallas as pl
from jax.experimental.pallas import tpu as pltpu
from jax.sharding import PartitionSpec as P

MESH = pl.DeviceIdType.MESH
BF16 = jnp.bfloat16
F32 = jnp.float32

D = 768
HEAD_DIM = 64
LEN = 1024
BLOCK = 256
PAIRS = BLOCK // 2
EPSILON = 1e-05
NEGATIVE = -1e30
ROOT_HALF = 0.7071067811865476
DENSITY_SCALE = 0.3989422804014327
VMEM_BYTES = 62 * 1024 * 1024


def dot(left, right):
    return jnp.dot(left, right, preferred_element_type=F32)


def dot_nt(left, right):
    return lax.dot_general(left, right, (((1,), (1,)), ((), ())), preferred_element_type=F32)


def columns_of(pairs):
    width = pairs.shape[1] // 2
    turned = pairs.T
    return jnp.concatenate([turned[:width], turned[width:]], axis=1)


def pairs_of(columns):
    half = columns.shape[1] // 2
    return jnp.concatenate([columns[:, :half], columns[:, half:]], axis=0).T


def vmem_spec():
    return pl.BlockSpec(memory_space=pltpu.VMEM)


def key_range(segment_ref, keep_ref, base, query_block, blocks):
    first = segment_ref[base + query_block * BLOCK]
    last = segment_ref[base + query_block * BLOCK + BLOCK - 1]
    low = jnp.int32(0)
    high = jnp.int32(-1)
    real = jnp.int32(-1)
    for block in range(blocks):
        low += (segment_ref[base + block * BLOCK + BLOCK - 1] < first).astype(jnp.int32)
        high += (segment_ref[base + block * BLOCK] <= last).astype(jnp.int32)
        real += (keep_ref[base + block * BLOCK] == 1).astype(jnp.int32)
    return low, jnp.minimum(high, jnp.maximum(real, query_block))


def block_bias(key_codes, codes_ref, query_block, key_block):
    keys = key_codes[pl.ds(pl.multiple_of(key_block * BLOCK, BLOCK), BLOCK), :]
    keys = jnp.concatenate([keys, keys], axis=1)
    queries = codes_ref[query_block, 0:1, :]
    place = lax.broadcasted_iota(jnp.int32, (BLOCK, BLOCK), 0) - lax.broadcasted_iota(
        jnp.int32, (BLOCK, BLOCK), 1
    )
    same = place == (query_block - key_block) * BLOCK
    return jnp.where((keys == queries) | same, 0.0, NEGATIVE)


def spread_key_codes(codes_ref, key_codes, blocks):
    for block in range(blocks):
        column = codes_ref[block].T[:, 1:2]
        key_codes[pl.ds(block * BLOCK, BLOCK), :] = jnp.broadcast_to(column, (BLOCK, 128))


def forward_kernel(
    segment_ref, keep_ref, inputs_ref, weight_ref, vectors_ref, codes_ref,
    turned_ref, joined_ref, context_ref, logsum_ref,
    key_codes, key_rows, value_rows, scaled, scores, totals, vector_columns,
):
    blocks = LEN // BLOCK
    base = pl.program_id(0) * LEN
    width = inputs_ref.shape[1] // 2
    heads = width // HEAD_DIM
    vector_columns[...] = vectors_ref[...].T
    spread_key_codes(codes_ref, key_codes, blocks)
    for block in range(blocks):
        turned = columns_of(inputs_ref[block * PAIRS : (block + 1) * PAIRS, :])
        turned_ref[block] = turned
        query = (dot(weight_ref[0], turned) + vector_columns[:, 0:1]).astype(BF16)
        key = dot(weight_ref[1], turned).astype(BF16)
        value = (dot(weight_ref[2], turned) + vector_columns[:, 1:2]).astype(BF16)
        joined_ref[block, 0] = query
        joined_ref[block, 1] = key
        joined_ref[block, 2] = value
        scaled[block] = query * jnp.array(HEAD_DIM ** (-0.5), BF16)
        for head in range(heads):
            rows = slice(head * HEAD_DIM, (head + 1) * HEAD_DIM)
            key_rows[head, block] = key[rows].T
            value_rows[head, block, :HEAD_DIM] = value[rows]
            value_rows[head, block, HEAD_DIM:] = jnp.ones((16, BLOCK), BF16)

    def query_step(query_block, carry):
        low, high = key_range(segment_ref, keep_ref, base, query_block, blocks)

        def score_step(key_block, highest):
            bias = block_bias(key_codes, codes_ref, query_block, key_block)
            fresh = []
            for head in range(heads):
                rows = slice(head * HEAD_DIM, (head + 1) * HEAD_DIM)
                score = dot(key_rows[head, key_block], scaled[query_block, rows, :]) + bias
                scores[head, key_block] = score
                fresh.append(
                    jnp.maximum(
                        highest[head], jnp.max(score.reshape(BLOCK // 8, 8, BLOCK), axis=0)
                    )
                )
            return tuple(fresh)

        start = jnp.full((8, BLOCK), 2 * NEGATIVE, F32)
        highest = lax.fori_loop(low, high + 1, score_step, (start,) * heads)
        highest = [jnp.max(part, axis=0, keepdims=True) for part in highest]
        totals[...] = jnp.zeros_like(totals)

        def value_step(key_block, carry):
            for head in range(heads):
                weights = jnp.exp(scores[head, key_block] - highest[head]).astype(BF16)
                totals[head] += dot(value_rows[head, key_block], weights)
            return carry

        lax.fori_loop(low, high + 1, value_step, 0)
        for head in range(heads):
            rows = slice(head * HEAD_DIM, (head + 1) * HEAD_DIM)
            total = totals[head, HEAD_DIM : HEAD_DIM + 1, :]
            context_ref[query_block, rows, :] = (totals[head, :HEAD_DIM, :] / total).astype(BF16)
            logsum_ref[query_block, head : head + 1, :] = highest[head] + jnp.log(total)
        return carry

    lax.fori_loop(0, blocks, query_step, 0)


def attention_forward(pairs, segment_ids, keep_mask, weight, vectors, codes):
    pair_count, doubled = pairs.shape
    width = doubled // 2
    heads = width // HEAD_DIM
    sequences = pair_count * 2 // LEN
    blocks = LEN // BLOCK
    every = sequences * blocks

    def whole(*shape):
        return pl.BlockSpec(shape, lambda i, *refs: (0,) * len(shape))

    def part(*shape):
        return pl.BlockSpec(shape, lambda i, *refs: (i,) + (0,) * (len(shape) - 1))

    return pl.pallas_call(
        forward_kernel,
        out_shape=(
            jax.ShapeDtypeStruct((every, width, BLOCK), BF16),
            jax.ShapeDtypeStruct((every, 3, width, BLOCK), BF16),
            jax.ShapeDtypeStruct((every, width, BLOCK), BF16),
            jax.ShapeDtypeStruct((every, 8, BLOCK), F32),
        ),
        grid_spec=pltpu.PrefetchScalarGridSpec(
            num_scalar_prefetch=2,
            grid=(sequences,),
            in_specs=[
                part(LEN // 2, doubled),
                whole(3, width, width),
                whole(*vectors.shape),
                part(blocks, 8, BLOCK),
            ],
            out_specs=(
                part(blocks, width, BLOCK),
                part(blocks, 3, width, BLOCK),
                part(blocks, width, BLOCK),
                part(blocks, 8, BLOCK),
            ),
            scratch_shapes=[
                pltpu.VMEM((LEN, 128), F32),
                pltpu.VMEM((heads, blocks, BLOCK, HEAD_DIM), BF16),
                pltpu.VMEM((heads, blocks, HEAD_DIM + 16, BLOCK), BF16),
                pltpu.VMEM((blocks, width, BLOCK), BF16),
                pltpu.VMEM((heads, blocks, BLOCK, BLOCK), F32),
                pltpu.VMEM((heads, HEAD_DIM + 16, BLOCK), F32),
                pltpu.VMEM((width, vectors.shape[0]), F32),
            ],
        ),
        compiler_params=pltpu.CompilerParams(vmem_limit_bytes=VMEM_BYTES),
        name="attention_forward",
    )(segment_ids, keep_mask, pairs, weight, vectors, codes)


def backward_kernel(
    segment_ref, keep_ref, turned_ref, joined_ref, context_ref, logsum_ref, upstream_ref,
    first_back_ref, weight_ref, codes_ref,
    input_grad_ref, weight_grad_ref, bias_grad_ref,
    key_codes, key_rows, value_rows, scaled, deltas, query_sum, key_sum, value_sum, weight_in,
):
    blocks = LEN // BLOCK
    step = pl.program_id(0)
    base = step * LEN
    width = turned_ref.shape[1]
    heads = width // HEAD_DIM
    scale = HEAD_DIM ** (-0.5)

    @pl.when(step == 0)
    def start():
        weight_grad_ref[...] = jnp.zeros_like(weight_grad_ref)
        bias_grad_ref[...] = jnp.zeros_like(bias_grad_ref)
        for kind in range(3):
            weight_in[kind] = weight_ref[kind].T

    spread_key_codes(codes_ref, key_codes, blocks)
    query_sum[...] = jnp.zeros_like(query_sum)
    key_sum[...] = jnp.zeros_like(key_sum)
    value_sum[...] = jnp.zeros_like(value_sum)
    for block in range(blocks):
        query = joined_ref[block, 0]
        scaled[block] = query * jnp.array(scale, BF16)
        product = upstream_ref[block].astype(F32) * context_ref[block].astype(F32)
        for head in range(heads):
            rows = slice(head * HEAD_DIM, (head + 1) * HEAD_DIM)
            key_rows[head, block] = joined_ref[block, 1, rows, :].T
            value_rows[head, block] = joined_ref[block, 2, rows, :].T
            deltas[block, head : head + 1, :] = jnp.sum(product[rows], axis=0, keepdims=True)

    def query_step(query_block, carry):
        low, high = key_range(segment_ref, keep_ref, base, query_block, blocks)

        def key_step(key_block, carry):
            bias = block_bias(key_codes, codes_ref, query_block, key_block)
            for head in range(heads):
                rows = slice(head * HEAD_DIM, (head + 1) * HEAD_DIM)
                query = scaled[query_block, rows, :]
                upstream = upstream_ref[query_block, rows, :]
                logsum = logsum_ref[query_block, head : head + 1, :]
                delta = deltas[query_block, head : head + 1, :]
                weights = jnp.exp(dot(key_rows[head, key_block], query) + bias - logsum)
                weight_back = dot(value_rows[head, key_block], upstream)
                score_back = (weights * (weight_back - delta)).astype(BF16)
                value_sum[key_block, rows, :] += dot_nt(upstream, weights.astype(BF16))
                key_sum[key_block, rows, :] += dot_nt(query, score_back)
                query_sum[query_block, rows, :] += dot(
                    joined_ref[key_block, 1, rows, :], score_back
                )
            return carry

        return lax.fori_loop(low, high + 1, key_step, carry)

    lax.fori_loop(0, blocks, query_step, 0)
    for block in range(blocks):
        query_low = (query_sum[block] * scale).astype(BF16)
        key_low = key_sum[block].astype(BF16)
        value_low = value_sum[block].astype(BF16)
        turned = turned_ref[block]
        weight_grad_ref[0] += dot_nt(query_low, turned)
        weight_grad_ref[1] += dot_nt(key_low, turned)
        weight_grad_ref[2] += dot_nt(value_low, turned)
        query_wide = query_low.astype(F32)
        value_wide = value_low.astype(F32)
        bias_grad_ref[0] += query_wide[:, :128] + query_wide[:, 128:]
        bias_grad_ref[1] += value_wide[:, :128] + value_wide[:, 128:]
        input_grad = (
            first_back_ref[block]
            + dot(weight_in[0], query_low)
            + dot(weight_in[1], key_low)
            + dot(weight_in[2], value_low)
        )
        input_grad_ref[block * PAIRS : (block + 1) * PAIRS, :] = pairs_of(input_grad)


def attention_backward(
    segment_ids, keep_mask, turned, joined, context, logsums, upstream, first_back, weight, codes
):
    every, width, unused = turned.shape
    heads = width // HEAD_DIM
    blocks = LEN // BLOCK
    sequences = every // blocks

    def whole(*shape):
        return pl.BlockSpec(shape, lambda i, *refs: (0,) * len(shape))

    def part(*shape):
        return pl.BlockSpec(shape, lambda i, *refs: (i,) + (0,) * (len(shape) - 1))

    return pl.pallas_call(
        backward_kernel,
        out_shape=(
            jax.ShapeDtypeStruct((sequences * LEN // 2, 2 * width), F32),
            jax.ShapeDtypeStruct((3, width, width), F32),
            jax.ShapeDtypeStruct((2, width, 128), F32),
        ),
        grid_spec=pltpu.PrefetchScalarGridSpec(
            num_scalar_prefetch=2,
            grid=(sequences,),
            in_specs=[
                part(blocks, width, BLOCK),
                part(blocks, 3, width, BLOCK),
                part(blocks, width, BLOCK),
                part(blocks, 8, BLOCK),
                part(blocks, width, BLOCK),
                part(blocks, width, BLOCK),
                whole(3, width, width),
                part(blocks, 8, BLOCK),
            ],
            out_specs=(
                part(LEN // 2, 2 * width),
                whole(3, width, width),
                whole(2, width, 128),
            ),
            scratch_shapes=[
                pltpu.VMEM((LEN, 128), F32),
                pltpu.VMEM((heads, blocks, BLOCK, HEAD_DIM), BF16),
                pltpu.VMEM((heads, blocks, BLOCK, HEAD_DIM), BF16),
                pltpu.VMEM((blocks, width, BLOCK), BF16),
                pltpu.VMEM((blocks, 8, BLOCK), F32),
                pltpu.VMEM((blocks, width, BLOCK), F32),
                pltpu.VMEM((blocks, width, BLOCK), F32),
                pltpu.VMEM((blocks, width, BLOCK), F32),
                pltpu.VMEM((3, width, width), BF16),
            ],
        ),
        compiler_params=pltpu.CompilerParams(vmem_limit_bytes=VMEM_BYTES),
        name="attention_backward",
    )(segment_ids, keep_mask, turned, joined, context, logsums, upstream, first_back, weight, codes)


def peer_of(axis, size, distance):
    return lax.rem(lax.axis_index(axis) + distance, size)


def source_of(axis, size, distance):
    return lax.rem(lax.axis_index(axis) + size - distance, size)


def greet(axes):
    barrier = pltpu.get_barrier_semaphore()
    count = 0
    for axis, size in axes:
        for distance in range(1, size):
            pl.semaphore_signal(
                barrier, inc=1, device_id={axis: peer_of(axis, size, distance)}, device_id_type=MESH
            )
            count += 1
    pl.semaphore_wait(barrier, count)


def remote(source, target, send_sem, recv_sem, axis, peer):
    return pltpu.make_async_remote_copy(
        src_ref=source, dst_ref=target, send_sem=send_sem, recv_sem=recv_sem,
        device_id={axis: peer}, device_id_type=MESH,
    )


def gather_kernel(rows, cols, query_ref, key_ref, value_ref, output_ref, joined_ref, output_all_ref, send, recv):
    row, col = lax.axis_index("row"), lax.axis_index("col")
    greet((("row", rows), ("col", cols)))
    copies = []
    for distance in range(1, rows):
        peer = peer_of("row", rows, distance)
        for kind, ref in enumerate((query_ref, key_ref, value_ref)):
            place = (kind, distance - 1)
            copies.append(remote(ref, joined_ref.at[kind, row], send.at[place], recv.at[place], "row", peer))
    for distance in range(1, cols):
        peer = peer_of("col", cols, distance)
        place = (3, distance - 1)
        copies.append(remote(output_ref, output_all_ref.at[col], send.at[place], recv.at[place], "col", peer))
    for copy in copies:
        copy.start()
    for kind, ref in enumerate((query_ref, key_ref, value_ref)):
        joined_ref[kind, row] = ref[...]
    output_all_ref[col] = output_ref[...]
    for copy in copies:
        copy.wait()


def gather_weights(rows, cols, query, key, value, output):
    part, width = query.shape
    return pl.pallas_call(
        functools.partial(gather_kernel, rows, cols),
        out_shape=(
            jax.ShapeDtypeStruct((3, rows, part, width), BF16),
            jax.ShapeDtypeStruct((cols,) + output.shape, BF16),
        ),
        in_specs=[vmem_spec()] * 4,
        out_specs=(vmem_spec(), vmem_spec()),
        scratch_shapes=[
            pltpu.SemaphoreType.DMA((4, max(rows, cols) - 1)),
            pltpu.SemaphoreType.DMA((4, max(rows, cols) - 1)),
        ],
        compiler_params=pltpu.CompilerParams(collective_id=0, has_side_effects=True),
        name="gather_weights",
    )(query, key, value, output)


ROWS = 32
QUERY_BIAS, VALUE_BIAS, OUTPUT_BIAS, FIRST_GAIN, FIRST_SHIFT, REDUCE_BIAS, SECOND_GAIN, SECOND_SHIFT, EXPAND_BIAS = range(9)
GAIN_SECOND, SHIFT_SECOND, BIAS_REDUCE, GAIN_FIRST, SHIFT_FIRST, BIAS_OUTPUT, BIAS_EXPAND = range(7)


def fold(value):
    return jnp.sum(value.reshape(value.shape[0] // 8, 8, value.shape[1]), axis=0)


def halves(value):
    return value[:, :128] + value[:, 128:]


def middle_kernel(
    rows, cols,
    turned_ref, context_ref, cotangent_ref, output_weight_ref, expand_weight_ref, reduce_weight_ref, vectors_ref,
    result_ref, first_back_ref, context_back_ref, grad_output_ref, grad_expand_ref, grad_reduce_ref, sums_ref,
    contexts, attended_out, attended_in, backs_out, backs_in, context_back_out,
    stat_out, stat_in, wide_out, wide_in, back_out, back_in,
    output_parts, expand_parts, reduce_parts,
    output_natural, output_turned, expand_natural, expand_turned, reduce_natural, reduce_turned,
    columns, first_sum, second_sum, middle_low, first_inverse, hidden, activated, slope,
    hidden_back, narrow, low_rows, cotangents,
    weight_send, weight_recv, send, recv,
):
    row, me = lax.axis_index("row"), lax.axis_index("col")
    width = turned_ref.shape[1]
    blocks = LEN // BLOCK
    chunks = turned_ref.shape[0] // blocks
    greet((("row", rows), ("col", cols)))

    kinds = ("contexts", "attended", "first", "second", "third", "backs", "context_back")

    def transfers(kind, chunk):
        made = []
        for distance in range(1, cols):
            peer = peer_of("col", cols, distance)
            place = (kinds.index(kind), chunk, distance - 1)
            if kind == "contexts":
                source, target = context_ref.at[chunk * blocks + peer], contexts.at[chunk, me]
            elif kind == "attended":
                source, target = attended_out.at[chunk, peer], attended_in.at[chunk, me]
            elif kind == "first":
                source, target = stat_out.at[chunk], stat_in.at[chunk, me]
            elif kind == "second":
                source, target = wide_out.at[chunk], wide_in.at[chunk, me]
            elif kind == "third":
                source, target = back_out.at[chunk], back_in.at[chunk, me]
            elif kind == "backs":
                source, target = backs_out.at[chunk * blocks + peer], backs_in.at[chunk, me]
            else:
                source, target = context_back_out.at[chunk, peer], context_back_ref.at[chunk * blocks + me]
            made.append(remote(source, target, send.at[place], recv.at[place], "col", peer))
        return made

    def begin(kind, chunk):
        for copy in transfers(kind, chunk):
            copy.start()

    def arrive(kind, chunk):
        for copy in transfers(kind, chunk):
            copy.wait_recv()

    for chunk in range(chunks):
        begin("contexts", chunk)
    weights = []
    for distance in range(1, rows):
        peer = peer_of("row", rows, distance)
        for kind, (source, target) in enumerate(
            ((output_weight_ref, output_parts), (expand_weight_ref, expand_parts), (reduce_weight_ref, reduce_parts))
        ):
            place = (kind, distance - 1)
            weights.append(
                remote(source, target.at[row], weight_send.at[place], weight_recv.at[place], "row", peer)
            )
    for kind in range(3):
        for copy in weights[kind::3]:
            copy.start()
    output_parts[row] = output_weight_ref[...]
    expand_parts[row] = expand_weight_ref[...]
    reduce_parts[row] = reduce_weight_ref[...]

    turned_vectors = vectors_ref[...].T
    for kind in range(columns.shape[0]):
        columns[kind] = jnp.broadcast_to(turned_vectors[:, kind : kind + 1], (width, 128))
    sums_ref[...] = jnp.zeros_like(sums_ref)
    grad_expand_ref[...] = jnp.zeros_like(grad_expand_ref)
    grad_reduce_ref[...] = jnp.zeros_like(grad_reduce_ref)
    for chunk in range(chunks):
        contexts[chunk, me] = context_ref[chunk * blocks + me]

    def turn_cotangent(block, carry):
        start = pl.multiple_of(block * PAIRS, PAIRS)
        cotangents[block] = columns_of(cotangent_ref[pl.ds(start, PAIRS), :])
        return carry

    lax.fori_loop(0, chunks * blocks, turn_cotangent, 0)

    def column(kind, at):
        part = columns[kind, pl.ds(at, ROWS), :]
        return jnp.concatenate([part, part], axis=1)

    def over_rows(count, body, carry):
        def step(index, carry):
            return body(pl.multiple_of(index * ROWS, ROWS), carry)

        return lax.fori_loop(0, count // ROWS, step, carry)

    def total(value):
        return jnp.sum(value, axis=0, keepdims=True)

    def add_sum(kind, at, value):
        sums_ref[kind, pl.ds(at, ROWS), :] += halves(value)

    def over_blocks(chunk, body):
        def step(block, carry):
            body(block, chunk * blocks + block)
            return carry

        lax.fori_loop(0, blocks, step, 0)

    zero = jnp.zeros((8, BLOCK), F32)

    def project(chunk):
        arrive("contexts", chunk)
        attended = dot(output_turned[...], contexts[chunk].reshape(cols * width, BLOCK))
        for group in range(cols):
            attended_out[chunk, group] = attended[group * width : (group + 1) * width].astype(BF16)
        begin("attended", chunk)
        attended_in[chunk, me] = attended_out[chunk, me]

    def add_first(chunk):
        arrive("attended", chunk)

        def body(block, place):
            def part(at, carry):
                here = pl.ds(at, ROWS)
                summed = (
                    turned_ref[place, here, :].astype(F32)
                    + attended_in[chunk, block, here, :].astype(F32)
                    + column(OUTPUT_BIAS, at)
                )
                first_sum[place, here, :] = summed
                return carry[0] + fold(summed), carry[1] + fold(summed * summed)

            one, two = over_rows(width, part, (zero, zero))
            stat_out[chunk, pl.ds(2 * block, 1), :] = total(one)
            stat_out[chunk, pl.ds(2 * block + 1, 1), :] = total(two)

        over_blocks(chunk, body)
        begin("first", chunk)

    def gathered(own, others, chunk, index):
        summed = jnp.zeros((1, BLOCK), F32)
        for source in range(cols):
            summed += others[chunk, source, pl.ds(index, 1), :]
        return summed

    def feed_forward(chunk):
        arrive("first", chunk)
        stat_in[chunk, me] = stat_out[chunk]

        def body(block, place):
            center = gathered(stat_out, stat_in, chunk, 2 * block) / D
            inverse = lax.rsqrt(
                gathered(stat_out, stat_in, chunk, 2 * block + 1) / D - center * center + EPSILON
            )
            first_inverse[place] = inverse

            def normalize(at, carry):
                here = pl.ds(at, ROWS)
                normal = (first_sum[place, here, :] - center) * inverse
                first_sum[place, here, :] = normal
                middle_low[place, here, :] = (
                    normal * column(FIRST_GAIN, at) + column(FIRST_SHIFT, at)
                ).astype(BF16)
                return carry

            over_rows(width, normalize, 0)
            hidden[...] = dot(expand_turned[...], middle_low[place])
            for quarter in range(hidden.shape[0] // width):

                def gelu(at, carry):
                    here = pl.ds(quarter * width + at, ROWS)
                    value = hidden[here, :] + column(EXPAND_BIAS + quarter, at)
                    share = 0.5 * (1.0 + lax.erf(value * ROOT_HALF))
                    activated[place, here, :] = (value * share).astype(BF16)
                    slope[place, here, :] = share + value * DENSITY_SCALE * jnp.exp(-0.5 * value * value)
                    return carry

                over_rows(width, gelu, 0)
            narrow[...] = dot(reduce_turned[...], activated[place])

            def add_second(at, carry):
                here = pl.ds(at, ROWS)
                middle = first_sum[place, here, :] * column(FIRST_GAIN, at) + column(FIRST_SHIFT, at)
                summed = middle + narrow[here, :] + column(REDUCE_BIAS, at)
                second_sum[place, here, :] = summed
                scaled = cotangents[place, here, :].astype(F32) * column(SECOND_GAIN, at)
                return (
                    carry[0] + fold(summed),
                    carry[1] + fold(summed * summed),
                    carry[2] + fold(scaled),
                    carry[3] + fold(scaled * summed),
                )

            found = over_rows(width, add_second, (zero,) * 4)
            for kind in range(4):
                wide_out[chunk, pl.ds(4 * block + kind, 1), :] = total(found[kind])

        over_blocks(chunk, body)
        begin("second", chunk)

    def feed_back(chunk):
        arrive("second", chunk)
        wide_in[chunk, me] = wide_out[chunk]

        def body(block, place):
            found = [gathered(wide_out, wide_in, chunk, 4 * block + kind) for kind in range(4)]
            center = found[0] / D
            inverse = lax.rsqrt(found[1] / D - center * center + EPSILON)
            mean_scaled = found[2] / D
            mean_product = inverse * (found[3] - center * found[2]) / D

            def back_norm(at, carry):
                here = pl.ds(at, ROWS)
                normal = (second_sum[place, here, :] - center) * inverse
                upstream = cotangents[place, here, :].astype(F32)
                gain = column(SECOND_GAIN, at)
                low_rows[here, :] = (normal * gain + column(SECOND_SHIFT, at)).astype(BF16)
                back = inverse * (upstream * gain - mean_scaled - normal * mean_product)
                second_sum[place, here, :] = back
                add_sum(GAIN_SECOND, at, upstream * normal)
                add_sum(SHIFT_SECOND, at, upstream)
                add_sum(BIAS_REDUCE, at, back)
                return carry

            over_rows(width, back_norm, 0)
            start = pl.multiple_of(place * PAIRS, PAIRS)
            result_ref[pl.ds(start, PAIRS), :] = pairs_of(low_rows[...])
            back_low = second_sum[place].astype(BF16)
            hidden[...] = dot(reduce_natural[...], back_low)
            for quarter in range(hidden.shape[0] // width):

                def back_gelu(at, carry):
                    here = pl.ds(quarter * width + at, ROWS)
                    back = (hidden[here, :] * slope[place, here, :]).astype(BF16)
                    hidden_back[here, :] = back
                    add_sum(BIAS_EXPAND + quarter, at, back.astype(F32))
                    return carry

                over_rows(width, back_gelu, 0)
            grad_reduce_ref[...] += dot_nt(back_low, activated[place])
            grad_expand_ref[...] += dot_nt(hidden_back[...], middle_low[place])
            narrow[...] = dot(expand_natural[...], hidden_back[...])

            def add_middle(at, carry):
                here = pl.ds(at, ROWS)
                back = second_sum[place, here, :] + narrow[here, :]
                second_sum[place, here, :] = back
                normal = first_sum[place, here, :]
                add_sum(GAIN_FIRST, at, back * normal)
                add_sum(SHIFT_FIRST, at, back)
                scaled = back * column(FIRST_GAIN, at)
                return carry[0] + fold(scaled), carry[1] + fold(scaled * normal)

            one, two = over_rows(width, add_middle, (zero, zero))
            back_out[chunk, pl.ds(2 * block, 1), :] = total(one)
            back_out[chunk, pl.ds(2 * block + 1, 1), :] = total(two)

        over_blocks(chunk, body)
        begin("third", chunk)

    def first_backward(chunk):
        arrive("third", chunk)
        back_in[chunk, me] = back_out[chunk]

        def body(block, place):
            mean_scaled = gathered(back_out, back_in, chunk, 2 * block) / D
            mean_product = gathered(back_out, back_in, chunk, 2 * block + 1) / D
            inverse = first_inverse[place]

            def part(at, carry):
                here = pl.ds(at, ROWS)
                back = inverse * (
                    second_sum[place, here, :] * column(FIRST_GAIN, at)
                    - mean_scaled
                    - first_sum[place, here, :] * mean_product
                )
                first_back_ref[place, here, :] = back
                backs_out[place, here, :] = back.astype(BF16)
                add_sum(BIAS_OUTPUT, at, back)
                return carry

            over_rows(width, part, 0)

        over_blocks(chunk, body)
        begin("backs", chunk)
        backs_in[chunk, me] = backs_out[chunk * blocks + me]

    def project_back(chunk):
        arrive("backs", chunk)
        back = dot(output_natural[...], backs_in[chunk].reshape(cols * width, BLOCK))
        for group in range(cols):
            context_back_out[chunk, group] = back[group * width : (group + 1) * width].astype(BF16)
        begin("context_back", chunk)
        context_back_ref[chunk * blocks + me] = context_back_out[chunk, me]
        every = contexts[chunk].reshape(cols * width, BLOCK)
        for part in range(rows):
            fresh = dot_nt(every, backs_in[chunk, part])
            if chunk == 0:
                grad_output_ref[part] = fresh
            else:
                grad_output_ref[part] += fresh

    for copy in weights[0::3]:
        copy.wait_recv()
    for group in range(cols):
        here = slice(group * width, (group + 1) * width)
        output_natural[here, :] = jnp.concatenate([output_parts[part, group] for part in range(rows)], axis=1)
    for part in range(rows):
        here = slice(part * width, (part + 1) * width)
        output_turned[here, :] = jnp.concatenate(
            [output_parts[part, group].T for group in range(cols)], axis=1
        )
    project(0)
    for copy in weights[1::3] + weights[2::3]:
        copy.wait_recv()
    expand_natural[...] = jnp.concatenate([expand_parts[part] for part in range(rows)], axis=1)
    for part in range(rows):
        expand_turned[part * width : (part + 1) * width, :] = expand_parts[part].T
    reduce_turned[...] = reduce_parts[...].reshape(reduce_turned.shape)
    reduce_natural[...] = reduce_turned[...].T
    project(1)
    project(2)
    add_first(0)
    feed_forward(0)
    add_first(1)
    feed_back(0)
    feed_forward(1)
    first_backward(0)
    add_first(2)
    feed_back(1)
    feed_forward(2)
    first_backward(1)
    project_back(0)
    feed_back(2)
    project_back(1)
    first_backward(2)
    project_back(2)
    for chunk in range(chunks):
        arrive("context_back", chunk)
    for copy in weights:
        copy.wait_send()
    for kind in kinds:
        for chunk in range(chunks):
            for copy in transfers(kind, chunk):
                copy.wait_send()


def middle_part(rows, cols, turned, context, cotangent, output_weight, expand_weight, reduce_weight, vectors):
    every, width, unused = turned.shape
    blocks = LEN // BLOCK
    chunks = every // blocks
    wide = expand_weight.shape[1] * rows
    most = max(rows, cols) - 1

    def low(*shape):
        return pltpu.VMEM(shape, BF16)

    def full(*shape):
        return pltpu.VMEM(shape, F32)

    return pl.pallas_call(
        functools.partial(middle_kernel, rows, cols),
        out_shape=(
            jax.ShapeDtypeStruct(cotangent.shape, BF16),
            jax.ShapeDtypeStruct((every, width, BLOCK), F32),
            jax.ShapeDtypeStruct((every, width, BLOCK), BF16),
            jax.ShapeDtypeStruct((rows, cols * width, width), F32),
            jax.ShapeDtypeStruct((wide, width), F32),
            jax.ShapeDtypeStruct((width, wide), F32),
            jax.ShapeDtypeStruct((6 + wide // width, width, 128), F32),
        ),
        in_specs=[vmem_spec()] * 7,
        out_specs=(vmem_spec(),) * 7,
        scratch_shapes=[
            low(chunks, cols, width, BLOCK), low(chunks, cols, width, BLOCK), low(chunks, cols, width, BLOCK),
            low(every, width, BLOCK), low(chunks, cols, width, BLOCK), low(chunks, cols, width, BLOCK),
            full(chunks, 2 * blocks, BLOCK), full(chunks, cols, 2 * blocks, BLOCK),
            full(chunks, 4 * blocks, BLOCK), full(chunks, cols, 4 * blocks, BLOCK),
            full(chunks, 2 * blocks, BLOCK), full(chunks, cols, 2 * blocks, BLOCK),
            low(rows, cols, width, width), low(rows, width, width), low(rows, *reduce_weight.shape),
            low(D, D), low(D, D), low(width, wide), low(wide, width), low(wide, width), low(width, wide),
            full(EXPAND_BIAS + wide // width, width, 128),
            full(every, width, BLOCK), full(every, width, BLOCK), low(every, width, BLOCK), full(every, 1, BLOCK),
            full(wide, BLOCK), low(every, wide, BLOCK), full(every, wide, BLOCK),
            low(wide, BLOCK), full(width, BLOCK), low(width, BLOCK), low(every, width, BLOCK),
            pltpu.SemaphoreType.DMA((3, most)), pltpu.SemaphoreType.DMA((3, most)),
            pltpu.SemaphoreType.DMA((7, chunks, most)), pltpu.SemaphoreType.DMA((7, chunks, most)),
        ],
        compiler_params=pltpu.CompilerParams(
            collective_id=1, has_side_effects=True, vmem_limit_bytes=VMEM_BYTES
        ),
        name="middle_part",
    )(turned, context, cotangent, output_weight, expand_weight, reduce_weight, vectors)


def reduce_kernel(
    devices, rows, cols,
    joined_ref, output_ref, expand_ref, reduce_ref, sums_ref, more_sums_ref,
    query_out_ref, key_out_ref, value_out_ref, output_out_ref, expand_out_ref, reduce_out_ref, vectors_out_ref,
    one_joined, one_output, one_expand, one_reduce, vectors_a,
    got_joined, got_output, got_expand, got_reduce, got_vectors_a,
    two_joined, two_output, two_expand, two_reduce, vectors_b,
    far_joined, far_output, far_expand, far_reduce, got_vectors_b,
    near_joined, near_output, near_expand, near_reduce,
    col_output, col_got, last_output, last_joined, last_expand, last_reduce, vectors_c,
    all_output, all_joined, all_expand, all_reduce, got_vectors_c,
    send, recv, col_send, col_recv, last_send, last_recv,
):
    row, col, data = lax.axis_index("row"), lax.axis_index("col"), lax.axis_index("dp")
    core, high = lax.rem(row, 2), row // 2
    sibling, across = row + 1 - 2 * core, lax.rem(row + 2, rows)
    width = expand_ref.shape[1]
    part = width // rows
    greet((("row", rows), ("col", cols), ("dp", devices)))

    def joined_piece(kind, owner):
        return joined_ref[kind, pl.ds(pl.multiple_of(owner * part, 8), part), :]

    def expand_piece(owner):
        return expand_ref[pl.ds(pl.multiple_of(owner * width, 8), width), :]

    def reduce_piece(owner):
        return reduce_ref[pl.ds(pl.multiple_of(owner * part, 8), part), :]

    for side in range(2):
        owner = 2 * side + 1 - core
        for kind in range(3):
            one_joined[side, kind] = joined_piece(kind, owner).astype(BF16)
        one_output[side] = output_ref[owner].astype(BF16)
        one_expand[side] = expand_piece(owner).astype(BF16)
        one_reduce[side] = reduce_piece(owner).astype(BF16)
    vectors_a[...] = jnp.zeros_like(vectors_a)
    gathered = [sums_ref[kind] for kind in range(sums_ref.shape[0])]
    gathered += [more_sums_ref[kind] for kind in range(more_sums_ref.shape[0])]
    for kind, value in enumerate(gathered):
        vectors_a[kind : kind + 1, :] = jnp.sum(value.T, axis=0, keepdims=True)
    first = [
        remote(source, target, send.at[0, index], recv.at[0, index], "row", sibling)
        for index, (source, target) in enumerate(
            ((one_output, got_output), (one_joined, got_joined), (one_expand, got_expand),
             (one_reduce, got_reduce), (vectors_a, got_vectors_a))
        )
    ]
    for copy in first:
        copy.start()
    for copy in first:
        copy.wait_recv()
    there, here = 1 - high, high
    far, near = 2 * there + core, 2 * here + core
    two_output[...] = (output_ref[far] + got_output[there].astype(F32)).astype(BF16)
    for kind in range(3):
        two_joined[kind] = (joined_piece(kind, far) + got_joined[there, kind].astype(F32)).astype(BF16)
    two_expand[...] = (expand_piece(far) + got_expand[there].astype(F32)).astype(BF16)
    two_reduce[...] = (reduce_piece(far) + got_reduce[there].astype(F32)).astype(BF16)
    vectors_b[...] = vectors_a[...] + got_vectors_a[...]
    second = [
        remote(source, target, send.at[1, index], recv.at[1, index], "row", across)
        for index, (source, target) in enumerate(
            ((two_output, far_output), (two_joined, far_joined), (two_expand, far_expand),
             (two_reduce, far_reduce), (vectors_b, got_vectors_b))
        )
    ]
    for copy in second:
        copy.start()
    near_output[...] = output_ref[near] + got_output[here].astype(F32)
    for kind in range(3):
        near_joined[kind] = joined_piece(kind, near) + got_joined[here, kind].astype(F32)
    near_expand[...] = expand_piece(near) + got_expand[here].astype(F32)
    near_reduce[...] = reduce_piece(near) + got_reduce[here].astype(F32)

    second[0].wait_recv()
    summed = near_output[...] + far_output[...].astype(F32)
    near_output[...] = summed
    for group in range(cols):
        col_output[group] = summed[group * width : (group + 1) * width].astype(BF16)
    across_cols = []
    for distance in range(1, cols):
        peer = peer_of("col", cols, distance)
        across_cols.append(
            remote(col_output.at[peer], col_got.at[col], col_send.at[distance - 1], col_recv.at[distance - 1], "col", peer)
        )
    for copy in across_cols:
        copy.start()

    for copy in second[1:]:
        copy.wait_recv()
    for kind in range(3):
        value = near_joined[kind] + far_joined[kind].astype(F32)
        near_joined[kind] = value
        last_joined[kind] = value.astype(BF16)
    value = near_expand[...] + far_expand[...].astype(F32)
    near_expand[...] = value
    last_expand[...] = value.astype(BF16)
    value = near_reduce[...] + far_reduce[...].astype(F32)
    near_reduce[...] = value
    last_reduce[...] = value.astype(BF16)
    vectors_c[...] = vectors_b[...] + got_vectors_b[...]
    last = []

    def exchange(index, source, target):
        for distance in range(1, devices):
            peer = peer_of("dp", devices, distance)
            copy = remote(
                source, target.at[data], last_send.at[index, distance - 1], last_recv.at[index, distance - 1], "dp", peer
            )
            copy.start()
            last.append(copy)

    exchange(1, last_joined, all_joined)
    exchange(2, last_expand, all_expand)
    exchange(3, last_reduce, all_reduce)
    exchange(4, vectors_c, got_vectors_c)

    for copy in across_cols:
        copy.wait_recv()
    own = near_output[pl.ds(pl.multiple_of(col * width, 8), width), :]
    for distance in range(1, cols):
        own += col_got[source_of("col", cols, distance)].astype(F32)
    last_output[...] = own.astype(BF16)
    exchange(0, last_output, all_output)
    for copy in last:
        copy.wait_recv()
    joined = [near_joined[kind] for kind in range(3)]
    expand, reduce, vectors = near_expand[...], near_reduce[...], vectors_c[...]
    for distance in range(1, devices):
        source = source_of("dp", devices, distance)
        own += all_output[source].astype(F32)
        joined = [joined[kind] + all_joined[source, kind].astype(F32) for kind in range(3)]
        expand += all_expand[source].astype(F32)
        reduce += all_reduce[source].astype(F32)
        vectors += got_vectors_c[source]
    query_out_ref[...] = joined[0]
    key_out_ref[...] = joined[1]
    value_out_ref[...] = joined[2]
    output_out_ref[...] = own
    expand_out_ref[...] = expand.T
    reduce_out_ref[...] = reduce
    vectors_out_ref[...] = vectors
    for copy in first + second + across_cols + last:
        copy.wait_send()


def reduce_gradients(devices, rows, cols, joined, output, expand, reduce, sums, more_sums):
    width = joined.shape[1]
    part = width // rows
    wide = expand.shape[0]
    count = 16

    def low(*shape):
        return pltpu.VMEM(shape, BF16)

    def full(*shape):
        return pltpu.VMEM(shape, F32)

    piece = (3, part, width)
    shapes = (piece, (cols * width, width), (width, width), (part, wide))
    vectors = (count, width)
    return pl.pallas_call(
        functools.partial(reduce_kernel, devices, rows, cols),
        out_shape=tuple(
            jax.ShapeDtypeStruct(shape, F32)
            for shape in ((part, width),) * 3 + ((width, width), (width, width), (part, wide), vectors)
        ),
        in_specs=[vmem_spec()] * 6,
        out_specs=(vmem_spec(),) * 7,
        scratch_shapes=[
            *(low(2, *shape) for shape in shapes), full(*vectors),
            *(low(2, *shape) for shape in shapes), full(*vectors),
            *(low(*shape) for shape in shapes), full(*vectors),
            *(low(*shape) for shape in shapes), full(*vectors),
            *(full(*shape) for shape in shapes),
            low(cols, width, width), low(cols, width, width),
            low(width, width), low(*piece), low(width, width), low(part, wide), full(*vectors),
            low(devices, width, width), low(devices, *piece), low(devices, width, width),
            low(devices, part, wide), full(devices, *vectors),
            pltpu.SemaphoreType.DMA((2, 5)), pltpu.SemaphoreType.DMA((2, 5)),
            pltpu.SemaphoreType.DMA((cols - 1,)), pltpu.SemaphoreType.DMA((cols - 1,)),
            pltpu.SemaphoreType.DMA((5, devices - 1)), pltpu.SemaphoreType.DMA((5, devices - 1)),
        ],
        compiler_params=pltpu.CompilerParams(
            collective_id=2, has_side_effects=True, vmem_limit_bytes=VMEM_BYTES
        ),
        name="reduce_gradients",
    )(joined, output, expand, reduce, sums, more_sums)


def local(
    devices, rows, cols,
    inputs, segment_ids, keep_mask, query_weight, query_bias, key_weight, value_weight, value_bias,
    output_weight, output_bias, first_gain, first_shift, expand_weight, expand_bias, reduce_weight,
    reduce_bias, second_gain, second_shift, cotangent,
):
    pairs, cotangent_pairs = inputs[:, 0, :], cotangent[:, 0, :]
    width = query_bias.shape[0]
    every = segment_ids.shape[0] // BLOCK
    coded = jnp.stack([segment_ids, jnp.where(keep_mask == 1, segment_ids, -1)]).astype(F32)
    coded = coded.reshape(2, every, PAIRS, 2).transpose(1, 0, 3, 2).reshape(every, 2, BLOCK)
    codes = jnp.pad(coded, ((0, 0), (0, 6), (0, 0)))
    stacked = [
        query_bias, value_bias, output_bias, first_gain, first_shift, reduce_bias, second_gain, second_shift,
    ]
    vectors = jnp.concatenate([jnp.stack(stacked), expand_bias.reshape(-1, width)])
    vectors = jnp.pad(vectors, ((0, -vectors.shape[0] % 8), (0, 0)))
    weight, output_blocks = gather_weights(
        rows, cols, query_weight.T, key_weight.T, value_weight.T, output_weight
    )
    weight = weight.reshape(3, width, width)
    turned, joined, context, logsums = attention_forward(pairs, segment_ids, keep_mask, weight, vectors, codes)
    result, first_back, context_back, grad_output, grad_expand, grad_reduce, sums = middle_part(
        rows, cols, turned, context, cotangent_pairs, output_blocks, expand_weight, reduce_weight.T, vectors
    )
    input_grad, grad_joined, more_sums = attention_backward(
        segment_ids, keep_mask, turned, joined, context, logsums, context_back, first_back, weight, codes
    )
    query, key, value, output, expand, reduce, found = reduce_gradients(
        devices, rows, cols, grad_joined, grad_output, grad_expand, grad_reduce, sums, more_sums
    )
    count = sums.shape[0]
    return (
        result[:, None, :], input_grad[:, None, :],
        query.T, found[count], key.T, value.T, found[count + 1], output, found[BIAS_OUTPUT],
        found[GAIN_FIRST], found[SHIFT_FIRST], expand, found[BIAS_EXPAND:count].reshape(-1), reduce.T,
        found[BIAS_REDUCE], found[GAIN_SECOND], found[SHIFT_SECOND],
    )


def solution(mesh):
    tokens, weight, vector = P(("dp", "row"), "col", None), P("col", "row"), P("col")
    ids = P(("dp", "row"))
    return jax.shard_map(
        functools.partial(local, mesh.shape["dp"], mesh.shape["row"], mesh.shape["col"]),
        mesh=mesh,
        in_specs=(
            tokens, ids, ids, weight, vector, weight, weight, vector, weight, vector, vector, vector, weight,
            vector, weight, vector, vector, vector, tokens,
        ),
        out_specs=(
            tokens, tokens, weight, vector, weight, weight, vector, weight, vector, vector, vector, weight,
            vector, weight, vector, vector, vector,
        ),
        check_vma=False,
    )
```

```python
import functools

import jax
import jax.numpy as jnp
from jax import lax
from jax.experimental import pallas as pl
from jax.experimental.pallas import tpu as pltpu
from jax.sharding import PartitionSpec as P

MESH = pl.DeviceIdType.MESH
BF16 = jnp.bfloat16
F32 = jnp.float32

D = 768
HEAD_DIM = 64
LEN = 1024
BLOCK = 256
PAIRS = BLOCK // 2
EPSILON = 1e-05
NEGATIVE = -1e30
ROOT_HALF = 0.7071067811865476
DENSITY_SCALE = 0.3989422804014327
VMEM_BYTES = 62 * 1024 * 1024


def dot(left, right):
    return jnp.dot(left, right, preferred_element_type=F32)


def dot_nt(left, right):
    return lax.dot_general(left, right, (((1,), (1,)), ((), ())), preferred_element_type=F32)


def columns_of(pairs):
    width = pairs.shape[1] // 2
    turned = pairs.T
    return jnp.concatenate([turned[:width], turned[width:]], axis=1)


def pairs_of(columns):
    half = columns.shape[1] // 2
    return jnp.concatenate([columns[:, :half], columns[:, half:]], axis=0).T


def vmem_spec():
    return pl.BlockSpec(memory_space=pltpu.VMEM)


def block_bias(key_codes, codes_ref, query_place, key_block, shift):
    keys = key_codes[key_block]
    keys = jnp.concatenate([keys, keys], axis=1)
    queries = codes_ref[query_place, 0:1, :]
    place = lax.broadcasted_iota(jnp.int32, (BLOCK, BLOCK), 0) - lax.broadcasted_iota(
        jnp.int32, (BLOCK, BLOCK), 1
    )
    return jnp.where((keys == queries) | (place == shift * BLOCK), 0.0, NEGATIVE)


def peer_of(axis, size, distance):
    return lax.rem(lax.axis_index(axis) + distance, size)


def source_of(axis, size, distance):
    return lax.rem(lax.axis_index(axis) + size - distance, size)


def greet(axes):
    barrier = pltpu.get_barrier_semaphore()
    count = 0
    for axis, size in axes:
        for distance in range(1, size):
            pl.semaphore_signal(
                barrier, inc=1, device_id={axis: peer_of(axis, size, distance)}, device_id_type=MESH
            )
            count += 1
    pl.semaphore_wait(barrier, count)


def remote(source, target, send_sem, recv_sem, axis, peer):
    return pltpu.make_async_remote_copy(
        src_ref=source, dst_ref=target, send_sem=send_sem, recv_sem=recv_sem,
        device_id={axis: peer}, device_id_type=MESH,
    )


ROWS = 32
QUERY_BIAS, VALUE_BIAS, OUTPUT_BIAS, FIRST_GAIN, FIRST_SHIFT, REDUCE_BIAS, SECOND_GAIN, SECOND_SHIFT, EXPAND_BIAS = range(9)
GAIN_SECOND, SHIFT_SECOND, BIAS_REDUCE, GAIN_FIRST, SHIFT_FIRST, BIAS_OUTPUT, BIAS_EXPAND = range(7)


def fold(value):
    return jnp.sum(value.reshape(value.shape[0] // 8, 8, value.shape[1]), axis=0)


def halves(value):
    return value[:, :128] + value[:, 128:]


def layer_kernel(
    devices, rows, cols,
    pairs_ref, cotangent_ref, codes_ref, vectors_ref, query_weight_ref, key_weight_ref, value_weight_ref,
    output_weight_ref, expand_weight_ref, reduce_weight_ref,
    result_ref, input_grad_ref, query_out_ref, key_out_ref, value_out_ref, output_out_ref, expand_out_ref,
    reduce_out_ref, vectors_out_ref,
    turned, joined, context, logsums, key_codes, key_rows, value_rows, value_turned, scaled, totals, deltas,
    joined_weight, joined_turned, joined_grad, context_back,
    grad_output, grad_expand, grad_reduce, sums,
    contexts, spread_out, spread_in,
    stat_out, stat_in, wide_out, wide_in, back_out, back_in,
    output_columns, output_parts, expand_parts, reduce_parts,
    output_natural, output_turned, expand_natural, expand_turned, reduce_natural, reduce_turned,
    columns, first_sum, second_sum, middle_low, first_inverse, hidden, activated, slope,
    hidden_back, narrow, low_rows,
    one_joined, one_output, one_expand, one_reduce, vectors_a,
    got_joined, got_output, got_expand, got_reduce, got_vectors_a,
    two_joined, two_output, two_expand, two_reduce, vectors_b,
    far_joined, far_output, far_expand, far_reduce, got_vectors_b,
    near_joined, near_output, near_expand, near_reduce,
    col_output, col_got, col_full, last_output, last_joined, last_expand, last_reduce, vectors_c,
    all_output, all_joined, all_expand, all_reduce, got_vectors_c,
    weight_send, weight_recv, send, recv, grad_send, grad_recv, col_send, col_recv, last_send, last_recv,
):
    row, me, data = lax.axis_index("row"), lax.axis_index("col"), lax.axis_index("dp")
    width = turned.shape[1]
    heads = width // HEAD_DIM
    blocks = LEN // BLOCK
    chunks = turned.shape[0] // blocks
    scale = HEAD_DIM ** (-0.5)
    greet((("row", rows), ("col", cols), ("dp", devices)))

    joined_copies, output_copies, other_copies, row_copies = [], [], [], []
    for distance in range(1, rows):
        peer = peer_of("row", rows, distance)
        for kind, ref in enumerate((query_weight_ref, key_weight_ref, value_weight_ref)):
            place = (kind, distance - 1)
            joined_copies.append(
                remote(ref, joined_weight.at[kind, row], weight_send.at[place], weight_recv.at[place], "row", peer)
            )
        for kind, source, target in ((3, expand_weight_ref, expand_parts), (4, reduce_weight_ref, reduce_parts)):
            place = (kind, distance - 1)
            other_copies.append(
                remote(source, target.at[row], weight_send.at[place], weight_recv.at[place], "row", peer)
            )
        place = (5, distance - 1)
        row_copies.append(
            remote(output_columns, output_parts.at[row], weight_send.at[place], weight_recv.at[place], "row", peer)
        )
    for distance in range(1, cols):
        peer = peer_of("col", cols, distance)
        place = (6, distance - 1)
        output_copies.append(
            remote(output_weight_ref, output_columns.at[me], weight_send.at[place], weight_recv.at[place], "col", peer)
        )
    for copy in joined_copies + output_copies + other_copies:
        copy.start()
    for kind, ref in enumerate((query_weight_ref, key_weight_ref, value_weight_ref)):
        joined_weight[kind, row] = ref[...]
    output_columns[me] = output_weight_ref[...]
    expand_parts[row] = expand_weight_ref[...]
    reduce_parts[row] = reduce_weight_ref[...]

    turned_vectors = vectors_ref[...].T
    for kind in range(columns.shape[0]):
        columns[kind] = jnp.broadcast_to(turned_vectors[:, kind : kind + 1], (width, 128))
    sums[...] = jnp.zeros_like(sums)
    grad_expand[...] = jnp.zeros_like(grad_expand)
    grad_reduce[...] = jnp.zeros_like(grad_reduce)
    joined_grad[...] = jnp.zeros_like(joined_grad)

    def turn(block, carry):
        here = pl.ds(pl.multiple_of(block * PAIRS, PAIRS), PAIRS)
        turned[block] = columns_of(pairs_ref[here, :])
        result_ref[block] = columns_of(cotangent_ref[here, :])
        return carry

    lax.fori_loop(0, chunks * blocks, turn, 0)

    def wide_column(kind):
        part = columns[kind]
        return jnp.concatenate([part, part], axis=1)

    def turn_heads(kind, target, block, place):
        for head in range(heads):
            target[head, block] = joined[place, kind, head * HEAD_DIM : (head + 1) * HEAD_DIM, :].T

    kinds = ("contexts", "attended", "first", "second", "third", "backs", "context_back")

    def transfers(kind, chunk):
        made = []
        for distance in range(1, cols):
            peer = peer_of("col", cols, distance)
            place = (kinds.index(kind), chunk, distance - 1)
            if kind == "contexts":
                source, target = context.at[chunk * blocks + peer], contexts.at[chunk, me]
            elif kind == "attended":
                source, target = spread_out.at[chunk, peer], spread_in.at[chunk, me]
            elif kind == "first":
                source, target = stat_out.at[chunk], stat_in.at[chunk, me]
            elif kind == "second":
                source, target = wide_out.at[chunk], wide_in.at[chunk, me]
            elif kind == "third":
                source, target = back_out.at[chunk], back_in.at[chunk, me]
            elif kind == "backs":
                source, target = middle_low.at[chunk * blocks + peer], spread_in.at[chunk, me]
            else:
                source, target = spread_out.at[chunk, peer], context_back.at[chunk * blocks + me]
            made.append(remote(source, target, send.at[place], recv.at[place], "col", peer))
        return made

    def begin(kind, chunk):
        for copy in transfers(kind, chunk):
            copy.start()

    def arrive(kind, chunk):
        for copy in transfers(kind, chunk):
            copy.wait_recv()

    def column(kind, at):
        part = columns[kind, pl.ds(at, ROWS), :]
        return jnp.concatenate([part, part], axis=1)

    def over_rows(count, body, carry):
        def step(index, carry):
            return body(pl.multiple_of(index * ROWS, ROWS), carry)

        return lax.fori_loop(0, count // ROWS, step, carry)

    def total(value):
        return jnp.sum(value, axis=0, keepdims=True)

    def add_sum(kind, at, value):
        sums[kind, pl.ds(at, ROWS), :] += halves(value)

    def over_blocks(chunk, body):
        def step(block, carry):
            body(block, chunk * blocks + block)
            return carry

        lax.fori_loop(0, blocks, step, 0)

    def attend(chunk):
        def make(block, carry):
            place = chunk * blocks + block
            rows_in = turned[place]
            query = (dot(joined_weight[0].reshape(width, width), rows_in) + wide_column(QUERY_BIAS)).astype(BF16)
            joined[place, 0] = query
            joined[place, 1] = dot(joined_weight[1].reshape(width, width), rows_in).astype(BF16)
            value = (dot(joined_weight[2].reshape(width, width), rows_in) + wide_column(VALUE_BIAS)).astype(BF16)
            joined[place, 2] = value
            scaled[block] = query * jnp.array(scale, BF16)
            key_codes[block] = jnp.broadcast_to(codes_ref[place].T[:, 1:2], (BLOCK, 128))
            turn_heads(1, key_rows, block, place)
            for head in range(heads):
                value_rows[head, block, :HEAD_DIM] = value[head * HEAD_DIM : (head + 1) * HEAD_DIM]
                value_rows[head, block, HEAD_DIM:] = jnp.ones((16, BLOCK), BF16)
            return carry

        lax.fori_loop(0, blocks, make, 0)

        def query_step(query_block, carry):
            here = chunk * blocks + query_block

            def score_step(key_block, highest):
                bias = block_bias(key_codes, codes_ref, here, key_block, query_block - key_block)
                fresh = []
                for head in range(heads):
                    rows_of = slice(head * HEAD_DIM, (head + 1) * HEAD_DIM)
                    score = dot(key_rows[head, key_block], scaled[query_block, rows_of, :]) + bias
                    first_sum[pl.ds(pl.multiple_of((head * blocks + key_block) * BLOCK, BLOCK), BLOCK), :] = score
                    fresh.append(
                        jnp.maximum(highest[head], jnp.max(score.reshape(BLOCK // 8, 8, BLOCK), axis=0))
                    )
                return tuple(fresh)

            low = jnp.full((8, BLOCK), 2 * NEGATIVE, F32)
            highest = lax.fori_loop(0, blocks, score_step, (low,) * heads)
            highest = [jnp.max(part, axis=0, keepdims=True) for part in highest]
            totals[...] = jnp.zeros_like(totals)

            def value_step(key_block, carry):
                for head in range(heads):
                    weights = jnp.exp(first_sum[pl.ds(pl.multiple_of((head * blocks + key_block) * BLOCK, BLOCK), BLOCK), :] - highest[head]).astype(BF16)
                    totals[head] += dot(value_rows[head, key_block], weights)
                return carry

            lax.fori_loop(0, blocks, value_step, 0)
            for head in range(heads):
                rows_of = slice(head * HEAD_DIM, (head + 1) * HEAD_DIM)
                whole = totals[head, HEAD_DIM : HEAD_DIM + 1, :]
                context[here, rows_of, :] = (totals[head, :HEAD_DIM, :] / whole).astype(BF16)
                logsums[here, head : head + 1, :] = highest[head] + jnp.log(whole)
            return carry

        lax.fori_loop(0, blocks, query_step, 0)
        begin("contexts", chunk)

    def attend_back(chunk):
        arrive("context_back", chunk)
        for kind in range(3):
            second_sum[kind * blocks : (kind + 1) * blocks] = jnp.zeros((blocks, width, BLOCK), F32)

        def make(block, carry):
            place = chunk * blocks + block
            scaled[block] = joined[place, 0] * jnp.array(scale, BF16)
            key_codes[block] = jnp.broadcast_to(codes_ref[place].T[:, 1:2], (BLOCK, 128))
            product = context_back[place].astype(F32) * context[place].astype(F32)
            turn_heads(1, key_rows, block, place)
            for head in range(heads):
                rows_of = slice(head * HEAD_DIM, (head + 1) * HEAD_DIM)
                value_turned[head, block] = joined[place, 2, rows_of, :].T
                deltas[block, head : head + 1, :] = jnp.sum(product[rows_of], axis=0, keepdims=True)
            return carry

        lax.fori_loop(0, blocks, make, 0)

        def pair_step(index, carry):
            query_block, key_block = index // blocks, lax.rem(index, blocks)
            query_place, key_place = chunk * blocks + query_block, chunk * blocks + key_block
            bias = block_bias(key_codes, codes_ref, query_place, key_block, query_block - key_block)
            for head in range(heads):
                rows_of = slice(head * HEAD_DIM, (head + 1) * HEAD_DIM)
                query = scaled[query_block, rows_of, :]
                upstream = context_back[query_place, rows_of, :]
                logsum = logsums[query_place, head : head + 1, :]
                delta = deltas[query_block, head : head + 1, :]
                weights = jnp.exp(dot(key_rows[head, key_block], query) + bias - logsum)
                weight_back = dot(value_turned[head, key_block], upstream)
                score_back = (weights * (weight_back - delta)).astype(BF16)
                second_sum[2 * blocks + key_block, rows_of, :] += dot_nt(upstream, weights.astype(BF16))
                second_sum[blocks + key_block, rows_of, :] += dot_nt(query, score_back)
                second_sum[query_block, rows_of, :] += dot(joined[key_place, 1, rows_of, :], score_back)
            return carry

        lax.fori_loop(0, blocks * blocks, pair_step, 0)

        def finish(block, carry):
            place = chunk * blocks + block
            query_low = (second_sum[block] * scale).astype(BF16)
            key_low = second_sum[blocks + block].astype(BF16)
            value_low = second_sum[2 * blocks + block].astype(BF16)
            rows_in = turned[place]
            joined_grad[0] += dot_nt(query_low, rows_in)
            joined_grad[1] += dot_nt(key_low, rows_in)
            joined_grad[2] += dot_nt(value_low, rows_in)
            sums[BIAS_EXPAND + (hidden.shape[0] // width)] += halves(query_low.astype(F32))
            sums[BIAS_EXPAND + (hidden.shape[0] // width) + 1] += halves(value_low.astype(F32))
            input_grad_ref[place] = (
                input_grad_ref[place]
                + dot(joined_turned[0], query_low)
                + dot(joined_turned[1], key_low)
                + dot(joined_turned[2], value_low)
            )
            return carry

        lax.fori_loop(0, blocks, finish, 0)

    zero = jnp.zeros((8, BLOCK), F32)

    def project(chunk):
        arrive("contexts", chunk)
        contexts[chunk, me] = context[chunk * blocks + me]
        attended = dot(output_turned[...], contexts[chunk].reshape(cols * width, BLOCK))
        for group in range(cols):
            spread_out[chunk, group] = attended[group * width : (group + 1) * width].astype(BF16)
        begin("attended", chunk)
        spread_in[chunk, me] = spread_out[chunk, me]

    def add_first(chunk):
        arrive("attended", chunk)

        def body(block, place):
            def part(at, carry):
                here = pl.ds(at, ROWS)
                summed = (
                    turned[place, here, :].astype(F32)
                    + spread_in[chunk, block, here, :].astype(F32)
                    + column(OUTPUT_BIAS, at)
                )
                first_sum[pl.ds(pl.multiple_of(place * width + at, ROWS), ROWS), :] = summed
                return carry[0] + fold(summed), carry[1] + fold(summed * summed)

            one, two = over_rows(width, part, (zero, zero))
            stat_out[chunk, pl.ds(2 * block, 1), :] = total(one)
            stat_out[chunk, pl.ds(2 * block + 1, 1), :] = total(two)

        over_blocks(chunk, body)
        begin("first", chunk)

    def gathered(own, others, chunk, index):
        summed = jnp.zeros((1, BLOCK), F32)
        for source in range(cols):
            summed += others[chunk, source, pl.ds(index, 1), :]
        return summed

    def feed_forward(chunk):
        arrive("first", chunk)
        stat_in[chunk, me] = stat_out[chunk]

        def body(block, place):
            center = gathered(stat_out, stat_in, chunk, 2 * block) / D
            inverse = lax.rsqrt(
                gathered(stat_out, stat_in, chunk, 2 * block + 1) / D - center * center + EPSILON
            )
            first_inverse[place] = inverse

            def normalize(at, carry):
                here = pl.ds(at, ROWS)
                normal = (first_sum[pl.ds(pl.multiple_of(place * width + at, ROWS), ROWS), :] - center) * inverse
                first_sum[pl.ds(pl.multiple_of(place * width + at, ROWS), ROWS), :] = normal
                middle_low[place, here, :] = (
                    normal * column(FIRST_GAIN, at) + column(FIRST_SHIFT, at)
                ).astype(BF16)
                return carry

            over_rows(width, normalize, 0)
            hidden[...] = dot(expand_turned[...], middle_low[place])
            for quarter in range(hidden.shape[0] // width):

                def gelu(at, carry):
                    here = pl.ds(quarter * width + at, ROWS)
                    value = hidden[here, :] + column(EXPAND_BIAS + quarter, at)
                    share = 0.5 * (1.0 + lax.erf(value * ROOT_HALF))
                    activated[place, here, :] = (value * share).astype(BF16)
                    slope[place, here, :] = (
                        share + value * DENSITY_SCALE * jnp.exp(-0.5 * value * value)
                    ).astype(BF16)
                    return carry

                over_rows(width, gelu, 0)
            narrow[...] = dot(reduce_turned[...], activated[place])

            def add_second(at, carry):
                here = pl.ds(at, ROWS)
                middle = first_sum[pl.ds(pl.multiple_of(place * width + at, ROWS), ROWS), :] * column(FIRST_GAIN, at) + column(FIRST_SHIFT, at)
                summed = middle + narrow[here, :] + column(REDUCE_BIAS, at)
                second_sum[place, here, :] = summed
                scaled = result_ref[place, here, :].astype(F32) * column(SECOND_GAIN, at)
                return (
                    carry[0] + fold(summed),
                    carry[1] + fold(summed * summed),
                    carry[2] + fold(scaled),
                    carry[3] + fold(scaled * summed),
                )

            found = over_rows(width, add_second, (zero,) * 4)
            for kind in range(4):
                wide_out[chunk, pl.ds(4 * block + kind, 1), :] = total(found[kind])

        over_blocks(chunk, body)
        begin("second", chunk)

    def feed_back(chunk):
        arrive("second", chunk)
        wide_in[chunk, me] = wide_out[chunk]

        def body(block, place):
            found = [gathered(wide_out, wide_in, chunk, 4 * block + kind) for kind in range(4)]
            center = found[0] / D
            inverse = lax.rsqrt(found[1] / D - center * center + EPSILON)
            mean_scaled = found[2] / D
            mean_product = inverse * (found[3] - center * found[2]) / D

            def back_norm(at, carry):
                here = pl.ds(at, ROWS)
                normal = (second_sum[place, here, :] - center) * inverse
                upstream = result_ref[place, here, :].astype(F32)
                gain = column(SECOND_GAIN, at)
                low_rows[here, :] = (normal * gain + column(SECOND_SHIFT, at)).astype(BF16)
                back = inverse * (upstream * gain - mean_scaled - normal * mean_product)
                second_sum[place, here, :] = back
                add_sum(GAIN_SECOND, at, upstream * normal)
                add_sum(SHIFT_SECOND, at, upstream)
                add_sum(BIAS_REDUCE, at, back)
                return carry

            over_rows(width, back_norm, 0)
            result_ref[place] = low_rows[...]
            back_low = second_sum[place].astype(BF16)
            hidden[...] = dot(reduce_natural[...], back_low)
            for quarter in range(hidden.shape[0] // width):

                def back_gelu(at, carry):
                    here = pl.ds(quarter * width + at, ROWS)
                    back = (hidden[here, :] * slope[place, here, :].astype(F32)).astype(BF16)
                    hidden_back[here, :] = back
                    add_sum(BIAS_EXPAND + quarter, at, back.astype(F32))
                    return carry

                over_rows(width, back_gelu, 0)
            grad_reduce[...] += dot_nt(back_low, activated[place])
            grad_expand[...] += dot_nt(hidden_back[...], middle_low[place])
            narrow[...] = dot(expand_natural[...], hidden_back[...])

            def add_middle(at, carry):
                here = pl.ds(at, ROWS)
                back = second_sum[place, here, :] + narrow[here, :]
                second_sum[place, here, :] = back
                normal = first_sum[pl.ds(pl.multiple_of(place * width + at, ROWS), ROWS), :]
                add_sum(GAIN_FIRST, at, back * normal)
                add_sum(SHIFT_FIRST, at, back)
                scaled = back * column(FIRST_GAIN, at)
                return carry[0] + fold(scaled), carry[1] + fold(scaled * normal)

            one, two = over_rows(width, add_middle, (zero, zero))
            back_out[chunk, pl.ds(2 * block, 1), :] = total(one)
            back_out[chunk, pl.ds(2 * block + 1, 1), :] = total(two)

        over_blocks(chunk, body)
        begin("third", chunk)

    def first_backward(chunk):
        arrive("third", chunk)
        back_in[chunk, me] = back_out[chunk]

        def body(block, place):
            mean_scaled = gathered(back_out, back_in, chunk, 2 * block) / D
            mean_product = gathered(back_out, back_in, chunk, 2 * block + 1) / D
            inverse = first_inverse[place]

            def part(at, carry):
                here = pl.ds(at, ROWS)
                back = inverse * (
                    second_sum[place, here, :] * column(FIRST_GAIN, at)
                    - mean_scaled
                    - first_sum[pl.ds(pl.multiple_of(place * width + at, ROWS), ROWS), :] * mean_product
                )
                input_grad_ref[place, here, :] = back
                middle_low[place, here, :] = back.astype(BF16)
                add_sum(BIAS_OUTPUT, at, back)
                return carry

            over_rows(width, part, 0)

        over_blocks(chunk, body)
        begin("backs", chunk)
        spread_in[chunk, me] = middle_low[chunk * blocks + me]

    def project_back(chunk):
        arrive("backs", chunk)
        for copy in transfers("attended", chunk):
            copy.wait_send()
        received = spread_in[chunk].reshape(cols * width, BLOCK)
        back = dot(output_natural[...], received)
        for group in range(cols):
            spread_out[chunk, group] = back[group * width : (group + 1) * width].astype(BF16)
        begin("context_back", chunk)
        context_back[chunk * blocks + me] = spread_out[chunk, me]
        every = contexts[chunk].reshape(cols * width, BLOCK)
        fresh = dot_nt(received, every)
        if chunk == 0:
            grad_output[...] = fresh
        else:
            grad_output[...] += fresh

    core, high = lax.rem(row, 2), row // 2
    sibling, opposite = row + 1 - 2 * core, lax.rem(row + 2, rows)
    there, side_here = 1 - high, high
    far, near = 2 * there + core, 2 * side_here + core
    portion = width // rows

    def portion_rows(owner):
        return pl.ds(pl.multiple_of(owner * portion, 8), portion)

    def piece(kind, owner):
        if kind == 0:
            return grad_output[pl.ds(pl.multiple_of(owner * width, 8), width), :]
        if kind == 1:
            return joined_grad[:, portion_rows(owner), :]
        if kind == 2:
            return grad_expand[pl.ds(pl.multiple_of(owner * width, 8), width), :]
        return grad_reduce[portion_rows(owner), :]

    one = (one_output, one_joined, one_expand, one_reduce, vectors_a)
    got = (got_output, got_joined, got_expand, got_reduce, got_vectors_a)
    two = (two_output, two_joined, two_expand, two_reduce, vectors_b)
    fars = (far_output, far_joined, far_expand, far_reduce, got_vectors_b)
    nears = (near_output, near_joined, near_expand, near_reduce, vectors_c)
    lasts = (last_output, last_joined, last_expand, last_reduce, vectors_c)
    alls = (all_output, all_joined, all_expand, all_reduce, got_vectors_c)

    def first_copy(kind):
        return remote(one[kind], got[kind], grad_send.at[0, kind], grad_recv.at[0, kind], "row", sibling)

    def second_copy(kind):
        return remote(two[kind], fars[kind], grad_send.at[1, kind], grad_recv.at[1, kind], "row", opposite)

    def col_copies():
        made = []
        for distance in range(1, cols):
            peer = peer_of("col", cols, distance)
            place = distance - 1
            made.append(remote(col_output.at[peer], col_got.at[me], col_send.at[place], col_recv.at[place], "col", peer))
        return made

    def last_copies(kind):
        made = []
        for distance in range(1, devices):
            peer = peer_of("dp", devices, distance)
            place = (kind, distance - 1)
            made.append(
                remote(lasts[kind], alls[kind].at[data], last_send.at[place], last_recv.at[place], "dp", peer)
            )
        return made

    def to_sibling(kinds_sent):
        for kind in kinds_sent:
            if kind == 4:
                vectors_a[...] = jnp.zeros_like(vectors_a)
                for index in range(sums.shape[0]):
                    vectors_a[index : index + 1, :] = jnp.sum(sums[index].T, axis=0, keepdims=True)
            else:
                for side in range(2):
                    one[kind][side] = piece(kind, 2 * side + 1 - core).astype(BF16)
            first_copy(kind).start()

    def to_opposite(kinds_sent):
        for kind in kinds_sent:
            first_copy(kind).wait_recv()
            if kind == 4:
                vectors_b[...] = vectors_a[...] + got_vectors_a[...]
            else:
                two[kind][...] = (piece(kind, far) + got[kind][there].astype(F32)).astype(BF16)
            second_copy(kind).start()
        for kind in kinds_sent:
            if kind != 4:
                nears[kind][...] = piece(kind, near) + got[kind][side_here].astype(F32)

    def to_data(kinds_sent):
        for kind in kinds_sent:
            second_copy(kind).wait_recv()
            if kind == 4:
                vectors_c[...] = vectors_b[...] + got_vectors_b[...]
            else:
                value = nears[kind][...] + fars[kind][...].astype(F32)
                nears[kind][...] = value
                lasts[kind][...] = value.astype(BF16)
            for copy in last_copies(kind):
                copy.start()

    def output_to_cols():
        second_copy(0).wait_recv()
        value = near_output[...] + far_output[...].astype(F32)
        for group in range(cols):
            own = value[:, group * width : (group + 1) * width]
            col_full[group] = own
            col_output[group] = own.astype(BF16)
        for copy in col_copies():
            copy.start()

    def output_to_data():
        for copy in col_copies():
            copy.wait_recv()
        value = col_full[me]
        for distance in range(1, cols):
            value += col_got[source_of("col", cols, distance)].astype(F32)
        col_full[me] = value
        last_output[...] = value.astype(BF16)
        for copy in last_copies(0):
            copy.start()

    def over_data(kind, value):
        for copy in last_copies(kind):
            copy.wait_recv()
        for distance in range(1, devices):
            value += alls[kind][source_of("dp", devices, distance)].astype(F32)
        return value

    for copy in joined_copies:
        copy.wait_recv()
    attend(0)
    for copy in output_copies:
        copy.wait_recv()
    for copy in row_copies:
        copy.start()
    output_parts[row] = output_columns[...]
    for kind in range(3):
        joined_turned[kind] = joined_weight[kind].reshape(width, width).T
    attend(1)
    for copy in row_copies:
        copy.wait_recv()
    for group in range(cols):
        here = slice(group * width, (group + 1) * width)
        output_natural[here, :] = jnp.concatenate([output_parts[part, group] for part in range(rows)], axis=1)
    for part in range(rows):
        here = slice(part * width, (part + 1) * width)
        output_turned[here, :] = jnp.concatenate(
            [output_parts[part, group].T for group in range(cols)], axis=1
        )
    project(0)
    attend(2)
    project(1)
    for copy in other_copies:
        copy.wait_recv()
    expand_natural[...] = jnp.concatenate([expand_parts[part] for part in range(rows)], axis=1)
    for part in range(rows):
        expand_turned[part * width : (part + 1) * width, :] = expand_parts[part].T
    reduce_turned[...] = reduce_parts[...].reshape(reduce_turned.shape)
    reduce_natural[...] = reduce_turned[...].T
    add_first(0)
    feed_forward(0)
    project(2)
    add_first(1)
    feed_back(0)
    feed_forward(1)
    first_backward(0)
    add_first(2)
    feed_back(1)
    feed_forward(2)
    first_backward(1)
    project_back(0)
    feed_back(2)
    project_back(1)
    first_backward(2)
    attend_back(0)
    project_back(2)
    to_sibling((0, 2, 3))
    attend_back(1)
    to_opposite((0, 2, 3))
    attend_back(2)
    to_sibling((1, 4))
    output_to_cols()
    to_data((2, 3))
    to_opposite((1, 4))
    output_to_data()
    to_data((1, 4))
    expand_out_ref[...] = over_data(2, near_expand[...]).T
    reduce_out_ref[...] = over_data(3, near_reduce[...])
    output_out_ref[...] = over_data(0, col_full[me]).T
    total_joined = over_data(1, near_joined[...])
    query_out_ref[...] = total_joined[0]
    key_out_ref[...] = total_joined[1]
    value_out_ref[...] = total_joined[2]
    vectors_out_ref[...] = over_data(4, vectors_c[...])
    for copy in joined_copies + output_copies + row_copies + other_copies + col_copies():
        copy.wait_send()
    for kind in kinds:
        for chunk in range(chunks):
            if kind != "attended":
                for copy in transfers(kind, chunk):
                    copy.wait_send()
    for kind in range(5):
        first_copy(kind).wait_send()
        second_copy(kind).wait_send()
        for copy in last_copies(kind):
            copy.wait_send()


def layer(devices, rows, cols, pairs, cotangent, codes, vectors, query, key, value, output, expand, reduce):
    width = output.shape[0]
    heads = width // HEAD_DIM
    every = pairs.shape[0] // PAIRS
    blocks = LEN // BLOCK
    chunks = every // blocks
    wide = expand.shape[1] * rows
    most = max(rows, cols) - 1
    part = width // rows
    count = 16
    kinds = BIAS_EXPAND + wide // width + 2

    def low(*shape):
        return pltpu.VMEM(shape, BF16)

    def full(*shape):
        return pltpu.VMEM(shape, F32)

    shapes = ((3, part, width), (width, cols * width), (width, width), (part, wide))
    dma = pltpu.SemaphoreType.DMA
    return pl.pallas_call(
        functools.partial(layer_kernel, devices, rows, cols),
        out_shape=(
            jax.ShapeDtypeStruct((every, width, BLOCK), BF16),
            jax.ShapeDtypeStruct((every, width, BLOCK), F32),
        ) + tuple(
            jax.ShapeDtypeStruct(shape, F32)
            for shape in ((part, width),) * 3 + ((width, width), (width, width), (part, wide), (count, width))
        ),
        in_specs=[vmem_spec()] * 10,
        out_specs=(vmem_spec(),) * 9,
        scratch_shapes=[
            low(every, width, BLOCK), low(every, 3, width, BLOCK), low(every, width, BLOCK), full(every, 8, BLOCK),
            full(blocks, BLOCK, 128), low(heads, blocks, BLOCK, HEAD_DIM), low(heads, blocks, HEAD_DIM + 16, BLOCK),
            low(heads, blocks, BLOCK, HEAD_DIM), low(blocks, width, BLOCK),
            full(heads, HEAD_DIM + 16, BLOCK), full(blocks, 8, BLOCK),
            low(3, rows, part, width), low(3, width, width), full(3, width, width),
            low(every, width, BLOCK),
            full(rows * width, cols * width), full(wide, width), full(width, wide), full(kinds, width, 128),
            low(chunks, cols, width, BLOCK), low(chunks, cols, width, BLOCK), low(chunks, cols, width, BLOCK),
            full(chunks, 2 * blocks, BLOCK), full(chunks, cols, 2 * blocks, BLOCK),
            full(chunks, 4 * blocks, BLOCK), full(chunks, cols, 4 * blocks, BLOCK),
            full(chunks, 2 * blocks, BLOCK), full(chunks, cols, 2 * blocks, BLOCK),
            low(cols, width, width), low(rows, cols, width, width), low(rows, width, width), low(rows, *reduce.shape),
            low(D, D), low(D, D), low(width, wide), low(wide, width), low(wide, width), low(width, wide),
            full(EXPAND_BIAS + wide // width, width, 128),
            full(max(every * width, heads * LEN), BLOCK), full(max(every, 3 * blocks), width, BLOCK),
            low(every, width, BLOCK), full(every, 1, BLOCK),
            full(wide, BLOCK), low(every, wide, BLOCK), low(every, wide, BLOCK),
            low(wide, BLOCK), full(width, BLOCK), low(width, BLOCK),
            *(low(2, *shape) for shape in shapes), full(count, width),
            *(low(2, *shape) for shape in shapes), full(count, width),
            *(low(*shape) for shape in shapes), full(count, width),
            *(low(*shape) for shape in shapes), full(count, width),
            *(full(*shape) for shape in shapes),
            low(cols, width, width), low(cols, width, width), full(cols, width, width),
            low(width, width), low(*shapes[0]), low(width, width), low(part, wide), full(count, width),
            low(devices, width, width), low(devices, *shapes[0]), low(devices, width, width),
            low(devices, part, wide), full(devices, count, width),
            dma((7, most)), dma((7, most)), dma((7, chunks, most)), dma((7, chunks, most)),
            dma((2, 5)), dma((2, 5)), dma((cols - 1,)), dma((cols - 1,)),
            dma((5, devices - 1)), dma((5, devices - 1)),
        ],
        compiler_params=pltpu.CompilerParams(
            collective_id=1, has_side_effects=True, vmem_limit_bytes=67043328
        ),
        name="layer",
    )(pairs, cotangent, codes, vectors, query, key, value, output, expand, reduce)


def finish_kernel(count, *refs):
    result_ref, grad_ref, vectors_ref = refs[:3]
    weights, outputs = refs[3:9], refs[9:]
    outputs[0][...] = pairs_of(result_ref[0])
    outputs[1][...] = pairs_of(grad_ref[0])

    @pl.when(pl.program_id(0) == 0)
    def once():
        for source, target in zip(weights, outputs[2:8]):
            target[...] = source[...]
        for kind in range(count):
            outputs[8 + kind][...] = vectors_ref[kind : kind + 1, :]


def finish_layer(result, grad, vectors, weights, count):
    every, width, unused = result.shape

    def whole(*shape):
        return pl.BlockSpec(shape, lambda i: (0,) * len(shape))

    block = pl.BlockSpec((1, width, BLOCK), lambda i: (i, 0, 0))
    pairs = pl.BlockSpec((PAIRS, 2 * width), lambda i: (i, 0))
    return pl.pallas_call(
        functools.partial(finish_kernel, count),
        out_shape=(
            jax.ShapeDtypeStruct((every * PAIRS, 2 * width), BF16),
            jax.ShapeDtypeStruct((every * PAIRS, 2 * width), F32),
            *(jax.ShapeDtypeStruct(weight.shape, F32) for weight in weights),
            *(jax.ShapeDtypeStruct((1, width), F32) for kind in range(count)),
        ),
        grid=(every,),
        in_specs=[block, block, whole(*vectors.shape)] + [whole(*weight.shape) for weight in weights],
        out_specs=(
            pairs, pairs, *(whole(*weight.shape) for weight in weights), *(whole(1, width) for kind in range(count)),
        ),
        name="finish_layer",
    )(result, grad, vectors, *weights)


def local(
    devices, rows, cols,
    inputs, segment_ids, keep_mask, query_weight, query_bias, key_weight, value_weight, value_bias,
    output_weight, output_bias, first_gain, first_shift, expand_weight, expand_bias, reduce_weight,
    reduce_bias, second_gain, second_shift, cotangent,
):
    width = query_bias.shape[0]
    every = segment_ids.shape[0] // BLOCK
    coded = jnp.stack([segment_ids, jnp.where(keep_mask == 1, segment_ids, -1)]).astype(F32)
    coded = coded.reshape(2, every, PAIRS, 2).transpose(1, 0, 3, 2).reshape(every, 2, BLOCK)
    codes = jnp.pad(coded, ((0, 0), (0, 6), (0, 0)))
    stacked = [
        query_bias, value_bias, output_bias, first_gain, first_shift, reduce_bias, second_gain, second_shift,
    ]
    vectors = jnp.concatenate([jnp.stack(stacked), expand_bias.reshape(-1, width)])
    vectors = jnp.pad(vectors, ((0, -vectors.shape[0] % 8), (0, 0)))
    result, grad, query, key, value, output, expand, reduce, found = layer(
        devices, rows, cols, inputs[:, 0, :], cotangent[:, 0, :], codes, vectors,
        query_weight.T, key_weight.T, value_weight.T, output_weight, expand_weight, reduce_weight.T,
    )
    quarters = expand_bias.shape[0] // width
    count = BIAS_EXPAND + quarters + 2
    finished = finish_layer(result, grad, found, (query, key, value, output, expand, reduce), count)
    result, grad, query, key, value, output, expand, reduce = finished[:8]
    found = [part[0] for part in finished[8:]]
    last = BIAS_EXPAND + quarters
    return (
        result[:, None, :], grad[:, None, :],
        query.T, found[last], key.T, value.T, found[last + 1], output, found[BIAS_OUTPUT],
        found[GAIN_FIRST], found[SHIFT_FIRST], expand, jnp.concatenate(found[BIAS_EXPAND:last]), reduce.T,
        found[BIAS_REDUCE], found[GAIN_SECOND], found[SHIFT_SECOND],
    )


def solution(mesh):
    tokens, weight, vector = P(("dp", "row"), "col", None), P("col", "row"), P("col")
    ids = P(("dp", "row"))
    return jax.shard_map(
        functools.partial(local, mesh.shape["dp"], mesh.shape["row"], mesh.shape["col"]),
        mesh=mesh,
        in_specs=(
            tokens, ids, ids, weight, vector, weight, weight, vector, weight, vector, vector, vector, weight,
            vector, weight, vector, vector, vector, tokens,
        ),
        out_specs=(
            tokens, tokens, weight, vector, weight, weight, vector, weight, vector, vector, vector, weight,
            vector, weight, vector, vector, vector,
        ),
        check_vma=False,
    )
```
